256 devices in a mesh: amp: 256 (over z, y, x, core).
Axes of the slice: x: 4, y: 4, z: 8, core: 2. Of those that a mesh axis runs over, the one named last changes fastest.
Arguments:
- ket_state: float32 [2, 8388608], P(None, 'amp'), may hold values from -6 to 6
- observable: float32 [8388608], P('amp'), may hold values from -6 to 6
- angles: float32 [2, 3], replicated, may hold values from -3.140625 to 3.140625
- gate_kinds: int32 [2, 32], replicated, may hold values from 0 to 2
Outputs:
- bra_state: float32 [2, 8388608], P(None, 'amp')
- grads: float32 [2, 3], replicated
The draws below stay inside these ranges and needn't reach their ends.
Inputs may be any that keep to these rules, and one draw needn't show every extreme that they name: `gate_kinds`: 0 and 1 name rotations about Y with angles[l, 0] and angles[l, 1], 2 a rotation about Z with angles[l, 2]; entries for qubits at or above the number of qubits are not used.
All inputs are finite; a program needn't handle non-finite values.
Results may differ from the reference program's by a relative error of at most 0.0003.
Values sent between devices are 32-bit elements; how exact they have to be, the bound alone decides.
A program may use at most 128 MiB of HBM per device.

```python
import math
import jax
import jax.numpy as jnp
from jax import lax

AMPS_DEV = 32768
LAYERS = 2
KINDS = 3
QSLOTS = 32
AMPS = 8388608
N_AMP = 256


def set_ends(drawn, own_key, smallest, largest):
    shape = drawn.shape
    place = [jax.random.randint(jax.random.fold_in(own_key, axis), (), 0, shape[axis]) for axis in range(len(shape))]
    drawn = drawn.at[tuple(place)].set(smallest)
    longest = shape.index(max(shape))
    place[longest] = (place[longest] + 1) % shape[longest]
    return drawn.at[tuple(place)].set(largest)


def block_levels(rng, dims, pieces, low, largest):
    def one(position, blocks):
        draws = jax.random.uniform(jax.random.fold_in(jax.random.fold_in(rng, 6), position), (blocks,), jnp.float32, low / len(pieces), largest / len(pieces))
        return jnp.repeat(jnp.exp(draws), dims[position] // blocks).reshape((-1,) + (1,) * (len(dims) - position - 1))

    factor_of = one(*pieces[0])
    for cut in pieces[1:]:
        factor_of = factor_of * one(*cut)
    return factor_of


def normal_values(stream_key, dims, spread, limit, cuts=(), kind=jnp.bfloat16):
    drawn = spread * jax.random.normal(stream_key, dims, jnp.float32)
    if cuts:
        drawn = drawn * block_levels(stream_key, dims, cuts, -0.22, 0.18)
    return jnp.clip(drawn, -limit, limit).astype(kind)


def setup_inputs(seed: int = 0) -> dict:
    streams_of = jax.random.split(jax.random.key(seed), 5)
    return {
        "ket_state": normal_values(streams_of[0], (2, AMPS), 1.0, 6.0, ((1, 256),), jnp.float32),
        "observable": normal_values(streams_of[1], (AMPS,), 1.0, 6.0, ((0, 256),), jnp.float32),
        "angles": jnp.clip(jax.random.uniform(streams_of[2], (LAYERS, KINDS), jnp.float32, -3.140625, 3.140625), -3.140625, 3.140625),
        "gate_kinds": set_ends(jax.random.randint(streams_of[3], (LAYERS, QSLOTS), 0, 3), jax.random.fold_in(streams_of[3], 1), 0, 2).astype(jnp.int32),
    }


def rotate_phase(values, cosine, sine_value):
    return jnp.stack([cosine * values[0] - sine_value * values[1], cosine * values[1] + sine_value * values[0]])

def undo_qubit(ket_state, bra_state, qubit_id, rotation, is_z):
    amp_total = ket_state.shape[1]
    fold_shape = (2, amp_total >> qubit_id + 1, 2, 1 << qubit_id)
    cosine = jnp.cos(0.5 * rotation)
    sine_value = jnp.sin(0.5 * rotation)

    def turn_y(operands):
        folded_ket, folded_bra = operands
        ket_low, ket_high = (folded_ket[:, :, 0], folded_ket[:, :, 1])
        bra_low, bra_high = (folded_bra[:, :, 0], folded_bra[:, :, 1])
        partial_value = 0.5 * jnp.sum(bra_high * ket_low - bra_low * ket_high)
        new_ket = jnp.stack([cosine * ket_low + sine_value * ket_high, cosine * ket_high - sine_value * ket_low], axis=2)
        new_bra = jnp.stack([cosine * bra_low + sine_value * bra_high, cosine * bra_high - sine_value * bra_low], axis=2)
        return (new_ket, new_bra, partial_value)

    def turn_z(operands):
        folded_ket, folded_bra = operands
        ket_low, ket_high = (folded_ket[:, :, 0], folded_ket[:, :, 1])
        bra_low, bra_high = (folded_bra[:, :, 0], folded_bra[:, :, 1])
        partial_value = 0.5 * (jnp.sum(bra_low[0] * ket_low[1] - bra_low[1] * ket_low[0]) - jnp.sum(bra_high[0] * ket_high[1] - bra_high[1] * ket_high[0]))
        new_ket = jnp.stack([rotate_phase(ket_low, cosine, sine_value), rotate_phase(ket_high, cosine, -sine_value)], axis=2)
        new_bra = jnp.stack([rotate_phase(bra_low, cosine, sine_value), rotate_phase(bra_high, cosine, -sine_value)], axis=2)
        return (new_ket, new_bra, partial_value)
    new_ket, new_bra, partial_value = lax.cond(is_z, turn_z, turn_y, (ket_state.reshape(fold_shape), bra_state.reshape(fold_shape)))
    return (new_ket.reshape(2, amp_total), new_bra.reshape(2, amp_total), partial_value)

def reference(ket_state, observable, angles, gate_kinds):
    amp_total = AMPS_DEV * N_AMP
    all_bits = int(amp_total).bit_length() - 1
    bra_state = 2.0 / math.sqrt(amp_total) * observable[None, :] * ket_state
    amp_index = jnp.arange(amp_total, dtype=jnp.int32)
    parity = jnp.zeros((amp_total,), jnp.int32)
    for qubit_id in range(all_bits):
        neighbor = (qubit_id + 1) % all_bits
        parity = parity + (amp_index >> qubit_id & 1) * (amp_index >> neighbor & 1)
    phase_sign = (1 - 2 * (parity & 1)).astype(jnp.float32)
    grads = jnp.zeros((LAYERS, KINDS), jnp.float32)
    kind_range = jnp.arange(KINDS)
    layer_range = jnp.arange(LAYERS)
    for layer_id in reversed(range(LAYERS)):
        ket_state = ket_state * phase_sign[None, :]
        bra_state = bra_state * phase_sign[None, :]
        for qubit_id in range(all_bits):
            kind_id = gate_kinds[layer_id, qubit_id]
            rotation = jnp.sum(jnp.where(kind_range == kind_id, angles[layer_id], 0.0))
            ket_state, bra_state, partial_value = undo_qubit(ket_state, bra_state, qubit_id, rotation, kind_id == 2)
            selector = ((layer_range[:, None] == layer_id) & (kind_range[None, :] == kind_id)).astype(grads.dtype)
            grads = grads + partial_value * selector
    return (bra_state, grads)
```

```python
import functools
import math

import jax
import jax.numpy as jnp
from jax import lax
from jax.experimental import pallas as pl
from jax.experimental.pallas import tpu as pltpu
from jax.sharding import PartitionSpec as P

MESH = pl.DeviceIdType.MESH
QUBITS = 23
LANE_QUBITS = (0, 1, 2, 3, 4, 13, 14)
HOME_ROWS = (7, 8, 9, 10, 11, 12, 5, 6)
AWAY_ROWS = (15, 16, 17, 18, 19, 20, 21, 22)
F32 = jnp.float32


def pair_mask(qubits):
    return sum(1 << q for q in qubits)


ALL_PAIRS = pair_mask(range(QUBITS))
LOCAL_PAIRS = pair_mask(range(14))
AWAY_PAIRS = pair_mask([0] + list(range(13, 23)))
REST_PAIRS = ALL_PAIRS - AWAY_PAIRS


def row_lane():
    row = lax.broadcasted_iota(jnp.int32, (256, 128), 0)
    lane = lax.broadcasted_iota(jnp.int32, (256, 128), 1)
    return row, lane


def entangle(me, away, pairs):
    row, lane = row_lane()
    own = me + jnp.zeros_like(row)
    far, near = (row, own) if away else (own, row)
    index = (lane & 31) | ((near >> 6) << 5) | ((near & 63) << 7) | ((lane >> 5) << 13) | (far << 15)
    both = index & ((index >> 1) | ((index & 1) << 22)) & pairs
    for shift in (16, 8, 4, 2, 1):
        both = both ^ (both >> shift)
    return (1 - 2 * (both & 1)).astype(F32)


def swap_bits(x, row_bit, lane_bit):
    rows = 1 << row_bit
    parts = x.reshape(256 // (2 * rows), 2, rows, 128)
    low, high = parts[:, 0].reshape(128, 128), parts[:, 1].reshape(128, 128)
    step = 1 << lane_bit
    lane = lax.broadcasted_iota(jnp.int32, (128, 128), 1)
    keep = (lane & step) == 0
    new_low = jnp.where(keep, low, pltpu.roll(high, step, 1))
    new_high = jnp.where(keep, pltpu.roll(low, 128 - step, 1), high)
    shape = (256 // (2 * rows), 1, rows, 128)
    return jnp.concatenate([new_low.reshape(shape), new_high.reshape(shape)], axis=1).reshape(256, 128)


def repack(x):
    return swap_bits(swap_bits(x, 6, 5), 7, 6)


def fold8(x):
    return jnp.sum(x.reshape(-1, 8, 128), axis=0)


def bit_sign(axis, position):
    place = lax.broadcasted_iota(jnp.int32, (8, 128), axis)
    return (1 - 2 * ((place >> position) & 1)).astype(F32)


def halves(x, position):
    parts = x.reshape(256 >> (position + 1), 2, 1 << position, 128)
    return parts[:, 0], parts[:, 1]


def flip(x, axis, position):
    step = 1 << position
    if axis == 0:
        y = x.reshape(32, 8, 128)
        place = lax.broadcasted_iota(jnp.int32, (32, 8, 128), 1)
        up, down = pltpu.roll(y, 8 - step, 1), pltpu.roll(y, step, 1)
        return jnp.where((place & step) == 0, up, down).reshape(256, 128)
    place = lax.broadcasted_iota(jnp.int32, (256, 128), 1)
    return jnp.where((place & step) == 0, pltpu.roll(x, 128 - step, 1), pltpu.roll(x, step, 1))


def terms(bra, ket, spots):
    bra_re, bra_im = bra
    ket_re, ket_im = ket
    cross = bra_re * ket_im - bra_im * ket_re
    total = fold8(cross)
    out = []
    for axis, position in spots:
        if axis == 0 and position >= 3:
            br0, br1 = halves(bra_re, position)
            bi0, bi1 = halves(bra_im, position)
            kr0, kr1 = halves(ket_re, position)
            ki0, ki1 = halves(ket_im, position)
            y_part = fold8(br1 * kr0 - br0 * kr1 + bi1 * ki0 - bi0 * ki1)
            c0, c1 = halves(cross, position)
            z_part = fold8(c0 - c1)
        else:
            sign = bit_sign(axis, position)
            pairs = bra_re * flip(ket_re, axis, position) + bra_im * flip(ket_im, axis, position)
            y_part = -sign * fold8(pairs)
            z_part = sign * total
        out.append((y_part, z_part))
    return out


def mm(a, b):
    return lax.dot_general(
        a, b, (((1,), (0,)), ((), ())), precision=lax.Precision.HIGHEST, preferred_element_type=F32
    )


def kernel(
    ket_hbm, obs_hbm, angles, kinds,
    bra_hbm, grads_ref,
    raw, send1, recv1, send2, recv2,
    theta, kind_tab, cos_tab, sy_tab, sz_tab,
    lane1, lane0, home1, home0, away1, away0,
    part, from_z, part_z, from_plane,
    in_sem, out_sem, send_sems, recv_sems,
):
    me = lax.axis_index("amp")
    z, y, x, c = me // 32, (me // 8) % 4, (me // 2) % 4, me % 2
    plane = me % 32
    inner = [((x + dx) % 4) * 2 + (c + dc) % 2 for dx in (2, 1, 3, 0) for dc in (0, 1)]
    tiers = [((y + dy) % 4) * 8 for dy in (2, 1, 3, 0)]

    def to_all(act):
        def body(step, carry):
            dz = jnp.where(step % 2 == 0, 4 + step // 2, 4 - (step + 1) // 2)
            base = ((z + dz) % 8) * 32
            for tier in tiers:
                for spot in inner:
                    act(base + tier + spot)
            return carry

        lax.fori_loop(0, 7, body, 0)
        for t, tier in enumerate(tiers):
            for s, spot in enumerate(inner):
                if (t, s) != (3, 6):
                    act(z * 32 + tier + spot)

    barrier = pltpu.get_barrier_semaphore()
    to_all(lambda d: pl.semaphore_signal(barrier, inc=1, device_id=(d,), device_id_type=MESH))

    loads = [
        pltpu.make_async_copy(ket_hbm.at[:, 0, :], raw.at[0], in_sem.at[0]),
        pltpu.make_async_copy(ket_hbm.at[:, 1, :], raw.at[1], in_sem.at[1]),
        pltpu.make_async_copy(obs_hbm, raw.at[2], in_sem.at[2]),
    ]
    for copy in loads:
        copy.start()

    theta[...] = jnp.zeros_like(theta)
    kind_tab[...] = jnp.zeros_like(kind_tab)
    picks = {}
    for layer in range(2):
        for q in range(QUBITS):
            kind = kinds[layer, q]
            picks[layer, q] = [jnp.where(kind == k, 1.0, 0.0).astype(F32) for k in range(3)]
            angle = jnp.where(
                kind == 0, angles[layer, 0], jnp.where(kind == 1, angles[layer, 1], angles[layer, 2])
            )
            row = layer * 24 + q
            theta[row : row + 1, :] = jnp.full((1, 128), 0.5 * angle, F32)
            kind_tab[row : row + 1, :] = jnp.full((1, 128), kind, jnp.int32)
    cos_tab[...] = jnp.cos(theta[...])
    sines = jnp.sin(theta[...])
    is_z = kind_tab[...] == 2
    sy_tab[...] = jnp.where(is_z, 0.0, sines)
    sz_tab[...] = jnp.where(is_z, sines, 0.0)

    def coefs(layer, q):
        row = slice(layer * 24 + q, layer * 24 + q + 1)
        return cos_tab[row, :], sy_tab[row, :], sz_tab[row, :]

    def kron(out_bits, in_bits, z_bits, layer, qubits, shape):
        real, imag = None, None
        for position, q in enumerate(qubits):
            cosine, sy, sz = coefs(layer, q)
            if shape[1] > 128:
                cosine, sy, sz = (jnp.concatenate([v, v], axis=1) for v in (cosine, sy, sz))
            b_out = (out_bits >> position) & 1
            b_in = (in_bits >> position) & 1
            same = b_out == b_in
            a = jnp.where(same, cosine, sy * (b_in - b_out).astype(F32))
            b = jnp.where(same, sz * (1 - 2 * b_out).astype(F32), 0.0)
            if real is None:
                real, imag = a, b
            else:
                real, imag = real * a - imag * b, real * b + imag * a
        return real, imag

    def build_lane(ref, layer):
        j = lax.broadcasted_iota(jnp.int32, (128, 128), 0)
        k = lax.broadcasted_iota(jnp.int32, (128, 128), 1)
        real, imag = kron(k, j, k, layer, LANE_QUBITS, (128, 128))
        ref[0:128, 0:128] = real
        ref[128:256, 128:256] = real
        ref[0:128, 128:256] = imag
        ref[128:256, 0:128] = -imag

    def build_rows(ref, layer, qubits):
        def body(block, carry):
            j = lax.broadcasted_iota(jnp.int32, (32, 256), 0) + block * 32
            k = lax.broadcasted_iota(jnp.int32, (32, 256), 1)
            real, imag = kron(j, k, j, layer, qubits, (32, 256))
            at = pl.ds(pl.multiple_of(block * 32, 32), 32)
            ref[0, at, :] = real
            ref[1, at, :] = imag
            return carry

        lax.fori_loop(0, 8, body, 0)

    def apply_lanes(x, ref):
        return mm(x, ref[...])

    def apply_rows(x, ref):
        a, b = mm(ref[0], x), mm(ref[1], x)
        return jnp.concatenate([a[:, :128] - b[:, 128:], a[:, 128:] + b[:, :128]], axis=1)

    def split(x):
        return x[:, :128], x[:, 128:]

    for copy in loads:
        copy.wait()
    for i in range(3):
        send1[i] = repack(raw[i])
    recv1[:, pl.ds(me, 1), :] = send1[:, pl.ds(me, 1), :]

    build_lane(lane1, 1)
    build_rows(home1, 1, HOME_ROWS)

    pl.semaphore_wait(barrier, 255)

    def exchange(source, target, slot):
        def act(d):
            pltpu.make_async_remote_copy(
                src_ref=source.at[:, pl.ds(d, 1), :],
                dst_ref=target.at[:, pl.ds(me, 1), :],
                send_sem=send_sems.at[slot],
                recv_sem=recv_sems.at[slot],
                device_id=(d,),
                device_id_type=MESH,
            ).start()

        to_all(act)
        return pltpu.make_async_remote_copy(
            src_ref=source.at[:, pl.ds(0, 255), :],
            dst_ref=target.at[:, pl.ds(0, 255), :],
            send_sem=send_sems.at[slot],
            recv_sem=recv_sems.at[slot],
            device_id=(me,),
            device_id_type=MESH,
        )

    first = exchange(send1, recv1, 0)

    scale = 2.0 / math.sqrt(1 << QUBITS)

    def start_state(ref, sign):
        ket_re, ket_im = ref[0] * sign, ref[1] * sign
        obs = ref[2] * scale
        return (obs * ket_re, obs * ket_im), (ket_re, ket_im)

    acc = {(layer, k): jnp.zeros((8, 128), F32) for layer in range(2) for k in range(3)}

    def tally(layer, qubits, values):
        for q, (y_part, z_part) in zip(qubits, values):
            pick = picks[layer, q]
            acc[layer, 0] = acc[layer, 0] + pick[0] * y_part
            acc[layer, 1] = acc[layer, 1] + pick[1] * y_part
            acc[layer, 2] = acc[layer, 2] + pick[2] * z_part

    spots = [(1, p) for p in range(7)] + [(0, p) for p in range(8)]
    local = list(LANE_QUBITS) + list(HOME_ROWS)
    bra, ket = start_state(send1, entangle(me, False, ALL_PAIRS))
    tally(1, local, terms(bra, ket, spots))
    local_sign = entangle(me, False, LOCAL_PAIRS)
    sign2 = jnp.concatenate([local_sign, local_sign], axis=1)

    def layer_one(state, rows_ref, sign2):
        x = jnp.concatenate(state, axis=1)
        return apply_rows(apply_lanes(x, lane1), rows_ref) * sign2

    bra1 = split(layer_one(bra, home1, sign2))
    ket1 = split(layer_one(ket, home1, sign2))
    inside = [(q, s) for q, s in zip(local, spots) if q not in (0, 14)]
    tally(0, [q for q, _ in inside], terms(bra1, ket1, [s for _, s in inside]))

    build_rows(away1, 1, AWAY_ROWS)
    build_rows(away0, 0, AWAY_ROWS)
    away_sign = entangle(me, True, AWAY_PAIRS)
    away2 = jnp.concatenate([away_sign, away_sign], axis=1)

    first.wait_recv()

    bra, ket = start_state(recv1, entangle(me, True, ALL_PAIRS))
    bra_x = layer_one(bra, away1, away2)
    done = apply_rows(bra_x, away0)
    send2[0], send2[1] = split(done)
    recv2[:, pl.ds(me, 1), :] = send2[:, pl.ds(me, 1), :]
    second = exchange(send2, recv2, 1)

    tally(1, AWAY_ROWS, terms(bra, ket, [(0, p) for p in range(8)]))
    ket_x = layer_one(ket, away1, away2)
    tally(
        0,
        list(AWAY_ROWS) + [0, 14],
        terms(split(bra_x), split(ket_x), [(0, p) for p in range(8)] + [(1, 0), (1, 6)]),
    )

    lane8 = lax.broadcasted_iota(jnp.int32, (8, 128), 1)
    mine = jnp.zeros((8, 128), F32)
    for layer in range(2):
        for k in range(3):
            value = 0.5 * jnp.sum(acc[layer, k], keepdims=True)
            mine = mine + jnp.where(lane8 == 3 * layer + k, value, 0.0)
    part[...] = mine
    from_z[pl.ds(z, 1)] = mine[None]
    peers_z = [((z + dz) % 8) * 32 + plane for dz in (4, 3, 5, 2, 6, 1, 7)]
    for d in peers_z:
        pltpu.make_async_remote_copy(
            src_ref=part, dst_ref=from_z.at[z], send_sem=send_sems.at[2], recv_sem=recv_sems.at[2],
            device_id=(d,), device_id_type=MESH,
        ).start()

    build_lane(lane0, 0)
    build_rows(home0, 0, HOME_ROWS)
    rest_sign = entangle(me, False, REST_PAIRS)
    rest2 = jnp.concatenate([rest_sign, rest_sign], axis=1)

    third = pltpu.make_async_remote_copy(
        src_ref=from_z.at[pl.ds(0, 7)], dst_ref=from_z.at[pl.ds(0, 7)],
        send_sem=send_sems.at[2], recv_sem=recv_sems.at[2], device_id=(me,), device_id_type=MESH,
    )
    third.wait_recv()
    summed = jnp.sum(from_z[...], axis=0)
    part_z[...] = summed
    from_plane[pl.ds(plane, 1)] = summed[None]
    for t, tier in enumerate(tiers):
        for s, spot in enumerate(inner):
            if (t, s) != (3, 6):
                pltpu.make_async_remote_copy(
                    src_ref=part_z, dst_ref=from_plane.at[plane],
                    send_sem=send_sems.at[3], recv_sem=recv_sems.at[3],
                    device_id=(z * 32 + tier + spot,), device_id_type=MESH,
                ).start()
    fourth = pltpu.make_async_remote_copy(
        src_ref=from_plane.at[pl.ds(0, 31)], dst_ref=from_plane.at[pl.ds(0, 31)],
        send_sem=send_sems.at[3], recv_sem=recv_sems.at[3], device_id=(me,), device_id_type=MESH,
    )

    second.wait_recv()
    x2 = jnp.concatenate([recv2[0], recv2[1]], axis=1)
    x2 = apply_rows(x2, home1) * rest2
    x2 = apply_rows(apply_lanes(x2, lane0), home0)
    re, im = split(x2)
    raw[0] = repack(re)
    raw[1] = repack(im)
    stores = [
        pltpu.make_async_copy(raw.at[0], bra_hbm.at[:, 0, :], out_sem.at[0]),
        pltpu.make_async_copy(raw.at[1], bra_hbm.at[:, 1, :], out_sem.at[1]),
    ]
    for copy in stores:
        copy.start()

    fourth.wait_recv()
    total = jnp.sum(from_plane[...], axis=0)
    grads_ref[...] = jnp.concatenate([total[0:1, 0:3], total[0:1, 3:6]], axis=0)
    for copy in (first, second, third, fourth):
        copy.wait_send()
    for copy in stores:
        copy.wait()


def on_device(ket_state, observable, angles, gate_kinds):
    ket = ket_state.reshape(2, 256, 128).transpose(1, 0, 2)
    obs = observable.reshape(256, 128)
    anywhere = pl.BlockSpec(memory_space=pl.ANY)
    scalars = pl.BlockSpec(memory_space=pltpu.SMEM)
    vmem = lambda *shape, dtype=F32: pltpu.VMEM(shape, dtype)
    bra, grads = pl.pallas_call(
        kernel,
        out_shape=(
            jax.ShapeDtypeStruct((256, 2, 128), F32),
            jax.ShapeDtypeStruct((2, 3), F32),
        ),
        in_specs=[anywhere, anywhere, scalars, scalars],
        out_specs=(anywhere, pl.BlockSpec(memory_space=pltpu.VMEM)),
        scratch_shapes=[
            vmem(3, 256, 128), vmem(3, 256, 128), vmem(3, 256, 128),
            vmem(2, 256, 128), vmem(2, 256, 128),
            vmem(48, 128), vmem(48, 128, dtype=jnp.int32),
            vmem(48, 128), vmem(48, 128), vmem(48, 128),
            vmem(256, 256), vmem(256, 256),
            vmem(2, 256, 256), vmem(2, 256, 256), vmem(2, 256, 256), vmem(2, 256, 256),
            vmem(8, 128), vmem(8, 8, 128), vmem(8, 128), vmem(32, 8, 128),
            pltpu.SemaphoreType.DMA((3,)), pltpu.SemaphoreType.DMA((2,)),
            pltpu.SemaphoreType.DMA((4,)), pltpu.SemaphoreType.DMA((4,)),
        ],
        compiler_params=pltpu.CompilerParams(collective_id=0, has_side_effects=True),
    )(ket, obs, angles, gate_kinds)
    return bra.transpose(1, 0, 2).reshape(2, 32768), grads


def solution(mesh):
    return jax.shard_map(
        on_device,
        mesh=mesh,
        in_specs=(P(None, "amp"), P("amp"), P(), P()),
        out_specs=(P(None, "amp"), P()),
        check_vma=False,
    )
```

```python
import functools
import math

import jax
import jax.numpy as jnp
from jax import lax
from jax.experimental import pallas as pl
from jax.experimental.pallas import tpu as pltpu
from jax.sharding import PartitionSpec as P

MESH = pl.DeviceIdType.MESH
QUBITS = 23
LANE_QUBITS = (0, 1, 2, 3, 4, 13, 14)
HOME_ROWS = (7, 8, 9, 10, 11, 12, 5, 6)
AWAY_ROWS = (15, 16, 17, 18, 19, 20, 21, 22)
F32 = jnp.float32


def pair_mask(qubits):
    return sum(1 << q for q in qubits)


ALL_PAIRS = pair_mask(range(QUBITS))
LOCAL_PAIRS = pair_mask(range(14))
AWAY_PAIRS = pair_mask([0] + list(range(13, 23)))
REST_PAIRS = ALL_PAIRS - AWAY_PAIRS


def row_lane():
    row = lax.broadcasted_iota(jnp.int32, (256, 128), 0)
    lane = lax.broadcasted_iota(jnp.int32, (256, 128), 1)
    return row, lane


def entangle(me, away, pairs):
    row, lane = row_lane()
    own = me + jnp.zeros_like(row)
    far, near = (row, own) if away else (own, row)
    index = (lane & 31) | ((near >> 6) << 5) | ((near & 63) << 7) | ((lane >> 5) << 13) | (far << 15)
    both = index & ((index >> 1) | ((index & 1) << 22)) & pairs
    for shift in (16, 8, 4, 2, 1):
        both = both ^ (both >> shift)
    return (1 - 2 * (both & 1)).astype(F32)


def swap_bits(x, row_bit, lane_bit):
    rows = 1 << row_bit
    parts = x.reshape(256 // (2 * rows), 2, rows, 128)
    low, high = parts[:, 0].reshape(128, 128), parts[:, 1].reshape(128, 128)
    step = 1 << lane_bit
    lane = lax.broadcasted_iota(jnp.int32, (128, 128), 1)
    keep = (lane & step) == 0
    new_low = jnp.where(keep, low, pltpu.roll(high, step, 1))
    new_high = jnp.where(keep, pltpu.roll(low, 128 - step, 1), high)
    shape = (256 // (2 * rows), 1, rows, 128)
    return jnp.concatenate([new_low.reshape(shape), new_high.reshape(shape)], axis=1).reshape(256, 128)


def repack(x):
    return swap_bits(swap_bits(x, 6, 5), 7, 6)


def fold8(x):
    return jnp.sum(x.reshape(-1, 8, 128), axis=0)


def bit_sign(axis, position):
    place = lax.broadcasted_iota(jnp.int32, (8, 128), axis)
    return (1 - 2 * ((place >> position) & 1)).astype(F32)


def halves(x, position):
    parts = x.reshape(256 >> (position + 1), 2, 1 << position, 128)
    return parts[:, 0], parts[:, 1]


def flip(x, axis, position):
    step = 1 << position
    if axis == 0:
        y = x.reshape(32, 8, 128)
        place = lax.broadcasted_iota(jnp.int32, (32, 8, 128), 1)
        up, down = pltpu.roll(y, 8 - step, 1), pltpu.roll(y, step, 1)
        return jnp.where((place & step) == 0, up, down).reshape(256, 128)
    place = lax.broadcasted_iota(jnp.int32, (256, 128), 1)
    return jnp.where((place & step) == 0, pltpu.roll(x, 128 - step, 1), pltpu.roll(x, step, 1))


def terms(bra, ket, spots):
    bra_re, bra_im = bra
    ket_re, ket_im = ket
    cross = bra_re * ket_im - bra_im * ket_re
    total = fold8(cross)
    out = []
    for axis, position in spots:
        if axis == 0 and position >= 3:
            br0, br1 = halves(bra_re, position)
            bi0, bi1 = halves(bra_im, position)
            kr0, kr1 = halves(ket_re, position)
            ki0, ki1 = halves(ket_im, position)
            y_part = fold8(br1 * kr0 - br0 * kr1 + bi1 * ki0 - bi0 * ki1)
            c0, c1 = halves(cross, position)
            z_part = fold8(c0 - c1)
        else:
            sign = bit_sign(axis, position)
            pairs = bra_re * flip(ket_re, axis, position) + bra_im * flip(ket_im, axis, position)
            y_part = -sign * fold8(pairs)
            z_part = sign * total
        out.append((y_part, z_part))
    return out


def cut(x):
    high = x.astype(jnp.bfloat16)
    return high, (x - high.astype(F32)).astype(jnp.bfloat16)


def mm(a, b):
    (a_high, a_low), (b_high, b_low) = a, b
    dot = functools.partial(jnp.dot, preferred_element_type=F32)
    return dot(a_high, b_high) + (dot(a_high, b_low) + dot(a_low, b_high))


def kernel(
    ket_hbm, obs_hbm, angles_hbm, kinds_hbm,
    bra_ref, grads_ref,
    angles, kinds, raw, send1, recv1, send2, recv2,
    theta, kind_tab, cos_tab, sy_tab, sz_tab,
    lane1, lane0, home1, home0, away1, away0,
    part, from_z, part_z, from_plane,
    in_sem, send_sems, recv_sems,
):
    me = lax.axis_index("amp")
    z, y, x, c = me // 32, (me // 8) % 4, (me // 2) % 4, me % 2
    plane = me % 32
    inner = [((x + dx) % 4) * 2 + (c + dc) % 2 for dx in (2, 1, 3, 0) for dc in (0, 1)]
    tiers = [((y + dy) % 4) * 8 for dy in (2, 1, 3, 0)]

    def to_all(act, begin=0, end=8):
        def body(step, carry):
            dz = jnp.where(step % 2 == 0, 4 + step // 2, 4 - (step + 1) // 2)
            base = ((z + dz) % 8) * 32
            for tier in tiers:
                for spot in inner:
                    act(base + tier + spot)
            return carry

        lax.fori_loop(begin, min(end, 7), body, 0)
        if end == 8:
            to_plane(lambda d, spot: act(d))

    def to_plane(act):
        for t, tier in enumerate(tiers):
            for s, spot in enumerate(inner):
                if (t, s) != (3, 6):
                    act(z * 32 + tier + spot, tier + spot)

    barrier = pltpu.get_barrier_semaphore()
    to_all(lambda d: pl.semaphore_signal(barrier, inc=1, device_id=(d,), device_id_type=MESH))

    loads = [
        pltpu.make_async_copy(ket_hbm.at[:, 0, :], raw.at[0], in_sem.at[0]),
        pltpu.make_async_copy(ket_hbm.at[:, 1, :], raw.at[1], in_sem.at[1]),
        pltpu.make_async_copy(obs_hbm, raw.at[2], in_sem.at[2]),
    ]
    settings = [
        pltpu.make_async_copy(angles_hbm, angles, in_sem.at[3]),
        pltpu.make_async_copy(kinds_hbm, kinds, in_sem.at[4]),
    ]
    for copy in loads + settings:
        copy.start()

    def coefs(layer, q):
        row = slice(layer * 24 + q, layer * 24 + q + 1)
        return cos_tab[row, :], sy_tab[row, :], sz_tab[row, :]

    def kron(out_bits, in_bits, z_bits, layer, qubits, shape):
        real, imag = None, None
        for position, q in enumerate(qubits):
            cosine, sy, sz = coefs(layer, q)
            if shape[1] > 128:
                cosine, sy, sz = (jnp.concatenate([v, v], axis=1) for v in (cosine, sy, sz))
            b_out = (out_bits >> position) & 1
            b_in = (in_bits >> position) & 1
            same = b_out == b_in
            a = jnp.where(same, cosine, sy * (b_in - b_out).astype(F32))
            b = jnp.where(same, sz * (1 - 2 * b_out).astype(F32), 0.0)
            if real is None:
                real, imag = a, b
            else:
                real, imag = real * a - imag * b, real * b + imag * a
        return real, imag

    def build_lane(ref, layer):
        j = lax.broadcasted_iota(jnp.int32, (128, 128), 0)
        k = lax.broadcasted_iota(jnp.int32, (128, 128), 1)
        real, imag = kron(k, j, k, layer, LANE_QUBITS, (128, 128))
        for i, (re, im) in enumerate(zip(cut(real), cut(imag))):
            ref[i, 0:128, 0:128] = re
            ref[i, 128:256, 128:256] = re
            ref[i, 0:128, 128:256] = im
            ref[i, 128:256, 0:128] = -im

    def build_rows(ref, layer, qubits):
        def body(block, carry):
            j = lax.broadcasted_iota(jnp.int32, (32, 256), 0) + block * 32
            k = lax.broadcasted_iota(jnp.int32, (32, 256), 1)
            real, imag = kron(j, k, j, layer, qubits, (32, 256))
            at = pl.ds(pl.multiple_of(block * 32, 32), 32)
            for i, (re, im) in enumerate(zip(cut(real), cut(imag))):
                ref[0, i, at, :] = re
                ref[1, i, at, :] = im
            return carry

        lax.fori_loop(0, 8, body, 0)

    def apply_lanes(x, ref):
        return mm(cut(x), (ref[0], ref[1]))

    def apply_rows(x, ref):
        x = cut(x)
        a, b = mm((ref[0, 0], ref[0, 1]), x), mm((ref[1, 0], ref[1, 1]), x)
        return jnp.concatenate([a[:, :128] - b[:, 128:], a[:, 128:] + b[:, :128]], axis=1)

    def split(x):
        return x[:, :128], x[:, 128:]

    for copy in loads:
        copy.wait()
    for i in range(3):
        send1[i] = repack(raw[i])
    recv1[:, pl.ds(me, 1), :] = send1[:, pl.ds(me, 1), :]

    pl.semaphore_wait(barrier, 255)

    def exchange(source, target, slot, begin=0, end=8):
        def act(d):
            pltpu.make_async_remote_copy(
                src_ref=source.at[:, pl.ds(d, 1), :],
                dst_ref=target.at[:, pl.ds(me, 1), :],
                send_sem=send_sems.at[slot],
                recv_sem=recv_sems.at[slot],
                device_id=(d,),
                device_id_type=MESH,
            ).start()

        to_all(act, begin, end)

    def exchanged(source, target, slot):
        return pltpu.make_async_remote_copy(
            src_ref=source.at[:, pl.ds(0, 255), :],
            dst_ref=target.at[:, pl.ds(0, 255), :],
            send_sem=send_sems.at[slot],
            recv_sem=recv_sems.at[slot],
            device_id=(me,),
            device_id_type=MESH,
        )

    exchange(send1, recv1, 0)
    first = exchanged(send1, recv1, 0)

    for copy in settings:
        copy.wait()
    theta[...] = jnp.zeros_like(theta)
    kind_tab[...] = jnp.zeros_like(kind_tab)
    picks = {}
    for layer in range(2):
        for q in range(QUBITS):
            kind = kinds[layer, q]
            picks[layer, q] = [jnp.where(kind == k, 1.0, 0.0).astype(F32) for k in range(3)]
            angle = jnp.where(
                kind == 0, angles[layer, 0], jnp.where(kind == 1, angles[layer, 1], angles[layer, 2])
            )
            row = layer * 24 + q
            theta[row : row + 1, :] = jnp.full((1, 128), 0.5 * angle, F32)
            kind_tab[row : row + 1, :] = jnp.full((1, 128), kind, jnp.int32)
    cos_tab[...] = jnp.cos(theta[...])
    sines = jnp.sin(theta[...])
    is_z = kind_tab[...] == 2
    sy_tab[...] = jnp.where(is_z, 0.0, sines)
    sz_tab[...] = jnp.where(is_z, sines, 0.0)

    build_lane(lane1, 1)
    build_rows(away1, 1, AWAY_ROWS)
    build_rows(away0, 0, AWAY_ROWS)
    build_rows(home1, 1, HOME_ROWS)

    scale = 2.0 / math.sqrt(1 << QUBITS)

    def start_state(ref, sign):
        ket_re, ket_im = ref[0] * sign, ref[1] * sign
        obs = ref[2] * scale
        return (obs * ket_re, obs * ket_im), (ket_re, ket_im)

    acc = {(layer, k): jnp.zeros((8, 128), F32) for layer in range(2) for k in range(3)}

    def tally(layer, qubits, values):
        for q, (y_part, z_part) in zip(qubits, values):
            pick = picks[layer, q]
            acc[layer, 0] = acc[layer, 0] + pick[0] * y_part
            acc[layer, 1] = acc[layer, 1] + pick[1] * y_part
            acc[layer, 2] = acc[layer, 2] + pick[2] * z_part

    spots = [(1, p) for p in range(7)] + [(0, p) for p in range(8)]
    local = list(LANE_QUBITS) + list(HOME_ROWS)
    bra, ket = start_state(send1, entangle(me, False, ALL_PAIRS))
    tally(1, local, terms(bra, ket, spots))
    local_sign = entangle(me, False, LOCAL_PAIRS)
    sign2 = jnp.concatenate([local_sign, local_sign], axis=1)

    def layer_one(state, rows_ref, sign2):
        x = jnp.concatenate(state, axis=1)
        return apply_rows(apply_lanes(x, lane1), rows_ref) * sign2

    bra1 = split(layer_one(bra, home1, sign2))
    ket1 = split(layer_one(ket, home1, sign2))
    inside = [(q, s) for q, s in zip(local, spots) if q not in (0, 14)]
    tally(0, [q for q, _ in inside], terms(bra1, ket1, [s for _, s in inside]))

    build_lane(lane0, 0)
    build_rows(home0, 0, HOME_ROWS)
    away_sign = entangle(me, True, AWAY_PAIRS)
    away2 = jnp.concatenate([away_sign, away_sign], axis=1)

    first.wait_recv()

    bra, ket = start_state(recv1, entangle(me, True, ALL_PAIRS))
    bra_x = layer_one(bra, away1, away2)
    done = apply_rows(bra_x, away0)
    send2[0], send2[1] = split(done)
    recv2[:, pl.ds(me, 1), :] = send2[:, pl.ds(me, 1), :]
    exchange(send2, recv2, 1, 0, 4)

    tally(1, AWAY_ROWS, terms(bra, ket, [(0, p) for p in range(8)]))
    ket_x = layer_one(ket, away1, away2)
    tally(
        0,
        list(AWAY_ROWS) + [0, 14],
        terms(split(bra_x), split(ket_x), [(0, p) for p in range(8)] + [(1, 0), (1, 6)]),
    )

    lane8 = lax.broadcasted_iota(jnp.int32, (8, 128), 1)
    mine = jnp.zeros((8, 128), F32)
    for layer in range(2):
        for k in range(3):
            value = 0.5 * jnp.sum(acc[layer, k], keepdims=True)
            mine = mine + jnp.where(lane8 == 3 * layer + k, value, 0.0)
    part[...] = mine
    from_plane[pl.ds(plane, 1)] = mine[None]

    def hand_over(d, spot):
        pltpu.make_async_remote_copy(
            src_ref=part, dst_ref=from_plane.at[plane], send_sem=send_sems.at[2], recv_sem=recv_sems.at[2],
            device_id=(d,), device_id_type=MESH,
        ).start()

    to_plane(hand_over)
    third = pltpu.make_async_remote_copy(
        src_ref=from_plane.at[pl.ds(0, 31)], dst_ref=from_plane.at[pl.ds(0, 31)],
        send_sem=send_sems.at[2], recv_sem=recv_sems.at[2], device_id=(me,), device_id_type=MESH,
    )
    exchange(send2, recv2, 1, 4, 8)
    second = exchanged(send2, recv2, 1)
    rest_sign = entangle(me, False, REST_PAIRS)
    rest2 = jnp.concatenate([rest_sign, rest_sign], axis=1)

    third.wait_recv()
    summed = jnp.sum(from_plane[...], axis=0)
    part_z[...] = summed
    from_z[pl.ds(z, 1)] = summed[None]
    for dz in (4, 3, 5, 2, 6, 1, 7):
        pltpu.make_async_remote_copy(
            src_ref=part_z, dst_ref=from_z.at[z], send_sem=send_sems.at[3], recv_sem=recv_sems.at[3],
            device_id=(((z + dz) % 8) * 32 + plane,), device_id_type=MESH,
        ).start()
    fourth = pltpu.make_async_remote_copy(
        src_ref=from_z.at[pl.ds(0, 7)], dst_ref=from_z.at[pl.ds(0, 7)],
        send_sem=send_sems.at[3], recv_sem=recv_sems.at[3], device_id=(me,), device_id_type=MESH,
    )

    second.wait_recv()
    x2 = jnp.concatenate([recv2[0], recv2[1]], axis=1)
    x2 = apply_rows(x2, home1) * rest2
    x2 = apply_rows(apply_lanes(x2, lane0), home0)
    bra_ref[0], bra_ref[1] = split(x2)

    fourth.wait_recv()
    grads_ref[...] = jnp.sum(from_z[...], axis=0)
    for copy in (first, second, third, fourth):
        copy.wait_send()


def finish(state, sums, bra_hbm, grads_ref, raw, out_sem):
    stores = []
    for i in range(2):
        raw[i] = repack(state[i])
        stores.append(pltpu.make_async_copy(raw.at[i], bra_hbm.at[:, i, :], out_sem.at[i]))
        stores[i].start()
    total = sums[0:1, :]
    grads_ref[...] = jnp.concatenate([total[:, 0:3], total[:, 3:6]], axis=0)
    for copy in stores:
        copy.wait()


def on_device(ket_state, observable, angles, gate_kinds):
    ket = ket_state.reshape(2, 256, 128).transpose(1, 0, 2)
    obs = observable.reshape(256, 128)
    main_memory = pl.BlockSpec(memory_space=pltpu.HBM)
    vmem = lambda *shape, dtype=F32: pltpu.VMEM(shape, dtype)
    half = lambda *shape: pltpu.VMEM(shape, jnp.bfloat16)
    on_chip = pl.BlockSpec(memory_space=pltpu.VMEM)
    state, sums = pl.pallas_call(
        kernel,
        out_shape=(
            jax.ShapeDtypeStruct((2, 256, 128), F32),
            jax.ShapeDtypeStruct((8, 128), F32),
        ),
        in_specs=[main_memory] * 4,
        out_specs=(on_chip, on_chip),
        scratch_shapes=[
            pltpu.SMEM((2, 3), F32), pltpu.SMEM((2, 32), jnp.int32),
            vmem(3, 256, 128), vmem(3, 256, 128), vmem(3, 256, 128),
            vmem(2, 256, 128), vmem(2, 256, 128),
            vmem(48, 128), vmem(48, 128, dtype=jnp.int32),
            vmem(48, 128), vmem(48, 128), vmem(48, 128),
            half(2, 256, 256), half(2, 256, 256),
            half(2, 2, 256, 256), half(2, 2, 256, 256), half(2, 2, 256, 256), half(2, 2, 256, 256),
            vmem(8, 128), vmem(8, 8, 128), vmem(8, 128), vmem(32, 8, 128),
            pltpu.SemaphoreType.DMA((5,)),
            pltpu.SemaphoreType.DMA((4,)), pltpu.SemaphoreType.DMA((4,)),
        ],
        compiler_params=pltpu.CompilerParams(
            collective_id=0, has_side_effects=True, vmem_limit_bytes=16 << 20
        ),
    )(*(pltpu.with_memory_space_constraint(v, pltpu.HBM) for v in (ket, obs, angles, gate_kinds)))
    bra, grads = pl.pallas_call(
        finish,
        out_shape=(
            jax.ShapeDtypeStruct((256, 2, 128), F32),
            jax.ShapeDtypeStruct((2, 3), F32),
        ),
        in_specs=[on_chip, on_chip],
        out_specs=(main_memory, on_chip),
        scratch_shapes=[vmem(2, 256, 128), pltpu.SemaphoreType.DMA((2,))],
        compiler_params=pltpu.CompilerParams(vmem_limit_bytes=4 << 20),
    )(state, sums)
    return bra.transpose(1, 0, 2).reshape(2, 32768), grads


def solution(mesh):
    return jax.shard_map(
        on_device,
        mesh=mesh,
        in_specs=(P(None, "amp"), P("amp"), P(), P()),
        out_specs=(P(None, "amp"), P()),
        check_vma=False,
    )
```

```python
import functools
import math

import jax
import jax.numpy as jnp
from jax import lax
from jax.experimental import pallas as pl
from jax.experimental.pallas import tpu as pltpu
from jax.sharding import PartitionSpec as P

MESH = pl.DeviceIdType.MESH
QUBITS = 23
LANE_QUBITS = (0, 1, 2, 3, 4, 13, 14)
HOME_ROWS = (7, 8, 9, 10, 11, 12, 5, 6)
AWAY_ROWS = (15, 16, 17, 18, 19, 20, 21, 22)
F32 = jnp.float32


def pair_mask(qubits):
    return sum(1 << q for q in qubits)


ALL_PAIRS = pair_mask(range(QUBITS))
LOCAL_PAIRS = pair_mask(range(14))
AWAY_PAIRS = pair_mask([0] + list(range(13, 23)))
REST_PAIRS = ALL_PAIRS - AWAY_PAIRS


def row_lane():
    row = lax.broadcasted_iota(jnp.int32, (256, 128), 0)
    lane = lax.broadcasted_iota(jnp.int32, (256, 128), 1)
    return row, lane


def entangle(me, pairs, chunk=None):
    row, lane = row_lane()
    own = me + jnp.zeros_like(row)
    far, near = (own, row) if chunk is None else (row, own)
    low = lane & 31 if chunk is None else (lane & 15) | (chunk << 4)
    index = low | ((near >> 6) << 5) | ((near & 63) << 7) | ((lane >> 5) << 13) | (far << 15)
    both = index & ((index >> 1) | ((index & 1) << 22)) & pairs
    for shift in (16, 8, 4, 2, 1):
        both = both ^ (both >> shift)
    return (1 - 2 * (both & 1)).astype(F32)


def swap_bits(x, row_bit, lane_bit):
    rows = 1 << row_bit
    parts = x.reshape(256 // (2 * rows), 2, rows, 128)
    low, high = parts[:, 0].reshape(128, 128), parts[:, 1].reshape(128, 128)
    step = 1 << lane_bit
    lane = lax.broadcasted_iota(jnp.int32, (128, 128), 1)
    keep = (lane & step) == 0
    new_low = jnp.where(keep, low, pltpu.roll(high, step, 1))
    new_high = jnp.where(keep, pltpu.roll(low, 128 - step, 1), high)
    shape = (256 // (2 * rows), 1, rows, 128)
    return jnp.concatenate([new_low.reshape(shape), new_high.reshape(shape)], axis=1).reshape(256, 128)


def repack(x):
    return swap_bits(swap_bits(x, 6, 5), 7, 6)


def lane_bit4():
    return (lax.broadcasted_iota(jnp.int32, (256, 128), 1) & 16) == 0


def up(x):
    return pltpu.roll(x, 16, 1)


def down(x):
    return pltpu.roll(x, 112, 1)


def to_chunks(real, imag):
    keep = lane_bit4()
    return jnp.where(keep, real, up(imag)), jnp.where(keep, down(real), imag)


def from_chunks(first, second):
    keep = lane_bit4()
    return jnp.where(keep, first, up(second)), jnp.where(keep, down(first), second)


def times_i(x):
    return jnp.where(lane_bit4(), -down(x), up(x))


def fold8(x):
    return jnp.sum(x.reshape(-1, 8, 128), axis=0)


def bit_sign(axis, position):
    place = lax.broadcasted_iota(jnp.int32, (8, 128), axis)
    return (1 - 2 * ((place >> position) & 1)).astype(F32)


def halves(x, position):
    parts = x.reshape(256 >> (position + 1), 2, 1 << position, 128)
    return parts[:, 0], parts[:, 1]


def flip(x, axis, position):
    step = 1 << position
    if axis == 0:
        y = x.reshape(32, 8, 128)
        place = lax.broadcasted_iota(jnp.int32, (32, 8, 128), 1)
        up, down = pltpu.roll(y, 8 - step, 1), pltpu.roll(y, step, 1)
        return jnp.where((place & step) == 0, up, down).reshape(256, 128)
    place = lax.broadcasted_iota(jnp.int32, (256, 128), 1)
    return jnp.where((place & step) == 0, pltpu.roll(x, 128 - step, 1), pltpu.roll(x, step, 1))


def terms(bras, kets, cross, spots):
    total = fold8(cross)
    out = []
    for axis, position in spots:
        if axis == 0 and position >= 3:
            y_part = 0.0
            for bra, ket in zip(bras, kets):
                b0, b1 = halves(bra, position)
                k0, k1 = halves(ket, position)
                y_part = y_part + (b1 * k0 - b0 * k1)
            y_part = fold8(y_part)
            c0, c1 = halves(cross, position)
            z_part = fold8(c0 - c1)
        else:
            sign = bit_sign(axis, position)
            pairs = sum(bra * flip(ket, axis, position) for bra, ket in zip(bras, kets))
            y_part = -sign * fold8(pairs)
            z_part = sign * total
        out.append((y_part, z_part))
    return out


def chunk_terms(bra, ket, spots):
    turned = flip(ket, 1, 4)
    cross = bra * jnp.where(lane_bit4(), turned, -turned)
    return terms([bra], [ket], cross, spots)


def home_terms(bra, ket, spots):
    return terms(bra, ket, bra[0] * ket[1] - bra[1] * ket[0], spots)


def cut(x):
    high = x.astype(jnp.bfloat16)
    return high, (x - high.astype(F32)).astype(jnp.bfloat16)


def mm(a, b):
    (a_high, a_low), (b_high, b_low) = a, b
    dot = functools.partial(jnp.dot, preferred_element_type=F32)
    return dot(a_high, b_high) + (dot(a_high, b_low) + dot(a_low, b_high))


def kernel(
    ket_hbm, obs_hbm, angles_hbm, kinds_hbm,
    bra_ref, grads_ref,
    angles, kinds, raw, send_a, send_b, recv_a, recv_b, send_c, send_d, recv_c, recv_d,
    theta, kind_tab, cos_tab, sy_tab, sz_tab,
    lane1, lane0, chunk_lane1, home1, home0, away1, away0,
    part, from_z, part_z, from_plane,
    in_sem, send_sems, recv_sems,
):
    me = lax.axis_index("amp")
    z, y, x, c = me // 32, (me // 8) % 4, (me // 2) % 4, me % 2
    plane = me % 32
    inner = [((x + dx) % 4) * 2 + (c + dc) % 2 for dx in (2, 1, 3, 0) for dc in (0, 1)]
    tiers = [((y + dy) % 4) * 8 for dy in (2, 1, 3, 0)]

    def to_all(act):
        def body(step, carry):
            dz = jnp.where(step % 2 == 0, 4 + step // 2, 4 - (step + 1) // 2)
            base = ((z + dz) % 8) * 32
            for tier in tiers:
                for spot in inner:
                    act(base + tier + spot)
            return carry

        lax.fori_loop(0, 7, body, 0)
        to_plane(lambda d, spot: act(d))

    def to_plane(act):
        for t, tier in enumerate(tiers):
            for s, spot in enumerate(inner):
                if (t, s) != (3, 6):
                    act(z * 32 + tier + spot, tier + spot)

    barrier = pltpu.get_barrier_semaphore()
    to_all(lambda d: pl.semaphore_signal(barrier, inc=1, device_id=(d,), device_id_type=MESH))

    loads = [
        pltpu.make_async_copy(ket_hbm.at[:, 0, :], raw.at[0], in_sem.at[0]),
        pltpu.make_async_copy(ket_hbm.at[:, 1, :], raw.at[1], in_sem.at[1]),
        pltpu.make_async_copy(obs_hbm, raw.at[2], in_sem.at[2]),
    ]
    settings = [
        pltpu.make_async_copy(angles_hbm, angles, in_sem.at[3]),
        pltpu.make_async_copy(kinds_hbm, kinds, in_sem.at[4]),
    ]
    for copy in loads + settings:
        copy.start()

    def coefs(layer, q):
        row = slice(layer * 24 + q, layer * 24 + q + 1)
        return cos_tab[row, :], sy_tab[row, :], sz_tab[row, :]

    def kron(value, out_bits, in_bits, layer, qubits):
        real, imag = value
        for position, q in qubits:
            cosine, sy, sz = coefs(layer, q)
            if out_bits.shape[1] > 128:
                cosine, sy, sz = (jnp.concatenate([v, v], axis=1) for v in (cosine, sy, sz))
            b_out = (out_bits >> position) & 1
            b_in = (in_bits >> position) & 1
            same = b_out == b_in
            a = jnp.where(same, cosine, sy * (b_in - b_out).astype(F32))
            b = jnp.where(same, sz * (1 - 2 * b_out).astype(F32), 0.0)
            if real is None:
                real, imag = a, b
            else:
                real, imag = real * a - imag * b, real * b + imag * a
        return real, imag

    def build_lane(ref, layer):
        j = lax.broadcasted_iota(jnp.int32, (128, 128), 0)
        k = lax.broadcasted_iota(jnp.int32, (128, 128), 1)
        real, imag = kron((None, None), k, j, layer, list(enumerate(LANE_QUBITS)))
        for i, (re, im) in enumerate(zip(cut(real), cut(imag))):
            ref[i, 0:128, 0:128] = re
            ref[i, 128:256, 128:256] = re
            ref[i, 0:128, 128:256] = im
            ref[i, 128:256, 0:128] = -im

    def build_chunk_lane(ref, layer):
        j = lax.broadcasted_iota(jnp.int32, (128, 128), 0)
        k = lax.broadcasted_iota(jnp.int32, (128, 128), 1)
        qubits = [(p, q) for p, q in enumerate(LANE_QUBITS) if p != 4]
        real, imag = kron((None, None), k, j, layer, qubits)
        part_in, part_out = (j >> 4) & 1, (k >> 4) & 1
        mixed = jnp.where(part_in == part_out, real, jnp.where(part_out == 1, imag, -imag))
        ref[0], ref[1] = cut(mixed)

    def build_rows(ref, layer, qubits):
        places = list(enumerate(qubits))
        j = lax.broadcasted_iota(jnp.int32, (32, 256), 0)
        k = lax.broadcasted_iota(jnp.int32, (32, 256), 1)
        base = kron((None, None), j, k, layer, places[:5])

        def body(block, carry):
            real, imag = kron(base, j + block * 32, k, layer, places[5:])
            at = pl.ds(pl.multiple_of(block * 32, 32), 32)
            for i, (re, im) in enumerate(zip(cut(real), cut(imag))):
                ref[0, i, at, :] = re
                ref[1, i, at, :] = im
            return carry

        lax.fori_loop(0, 8, body, 0)

    def apply_lanes(x, ref):
        return mm(cut(x), (ref[0], ref[1]))

    def apply_rows(x, ref):
        x = cut(x)
        a, b = mm((ref[0, 0], ref[0, 1]), x), mm((ref[1, 0], ref[1, 1]), x)
        return jnp.concatenate([a[:, :128] - b[:, 128:], a[:, 128:] + b[:, :128]], axis=1)

    def apply_chunk_rows(x, ref):
        x = cut(x)
        return mm((ref[0, 0], ref[0, 1]), x) + times_i(mm((ref[1, 0], ref[1, 1]), x))

    def split(x):
        return x[:, :128], x[:, 128:]

    for copy in loads:
        copy.wait()
    for i in range(3):
        raw[i] = repack(raw[i])
    send_a[0], send_b[0] = to_chunks(raw[0], raw[1])
    send_a[1] = raw[2]

    def keep_own(source, target):
        target[:, pl.ds(me, 1), :] = source[:, pl.ds(me, 1), :]

    keep_own(send_a, recv_a)
    keep_own(send_b, recv_b)

    pl.semaphore_wait(barrier, 255)

    def exchange(source, target, slot):
        def act(d):
            pltpu.make_async_remote_copy(
                src_ref=source.at[:, pl.ds(d, 1), :],
                dst_ref=target.at[:, pl.ds(me, 1), :],
                send_sem=send_sems.at[slot],
                recv_sem=recv_sems.at[slot],
                device_id=(d,),
                device_id_type=MESH,
            ).start()

        to_all(act)

    def exchanged(source, target, slot):
        return pltpu.make_async_remote_copy(
            src_ref=source.at[:, pl.ds(0, 255), :],
            dst_ref=target.at[:, pl.ds(0, 255), :],
            send_sem=send_sems.at[slot],
            recv_sem=recv_sems.at[slot],
            device_id=(me,),
            device_id_type=MESH,
        )

    exchange(send_a, recv_a, 0)
    exchange(send_b, recv_b, 1)
    out_a = exchanged(send_a, recv_a, 0)
    out_b = exchanged(send_b, recv_b, 1)

    for copy in settings:
        copy.wait()
    theta[...] = jnp.zeros_like(theta)
    kind_tab[...] = jnp.zeros_like(kind_tab)
    picks = {}
    for layer in range(2):
        for q in range(QUBITS):
            kind = kinds[layer, q]
            picks[layer, q] = [jnp.where(kind == k, 1.0, 0.0).astype(F32) for k in range(3)]
            angle = jnp.where(
                kind == 0, angles[layer, 0], jnp.where(kind == 1, angles[layer, 1], angles[layer, 2])
            )
            row = layer * 24 + q
            theta[row : row + 1, :] = jnp.full((1, 128), 0.5 * angle, F32)
            kind_tab[row : row + 1, :] = jnp.full((1, 128), kind, jnp.int32)
    cos_tab[...] = jnp.cos(theta[...])
    sines = jnp.sin(theta[...])
    is_z = kind_tab[...] == 2
    sy_tab[...] = jnp.where(is_z, 0.0, sines)
    sz_tab[...] = jnp.where(is_z, sines, 0.0)

    build_chunk_lane(chunk_lane1, 1)
    build_rows(away1, 1, AWAY_ROWS)
    build_rows(away0, 0, AWAY_ROWS)
    build_lane(lane1, 1)
    build_rows(home1, 1, HOME_ROWS)

    scale = 2.0 / math.sqrt(1 << QUBITS)

    acc = {(layer, k): jnp.zeros((8, 128), F32) for layer in range(2) for k in range(3)}

    def tally(layer, qubits, values):
        for q, (y_part, z_part) in zip(qubits, values):
            pick = picks[layer, q]
            acc[layer, 0] = acc[layer, 0] + pick[0] * y_part
            acc[layer, 1] = acc[layer, 1] + pick[1] * y_part
            acc[layer, 2] = acc[layer, 2] + pick[2] * z_part

    spots = [(1, p) for p in range(7)] + [(0, p) for p in range(8)]
    local = list(LANE_QUBITS) + list(HOME_ROWS)
    sign = entangle(me, ALL_PAIRS)
    ket = (raw[0] * sign, raw[1] * sign)
    bra = tuple(raw[2] * scale * part for part in ket)
    tally(1, local, home_terms(bra, ket, spots))
    local_sign = entangle(me, LOCAL_PAIRS)
    sign2 = jnp.concatenate([local_sign, local_sign], axis=1)

    def home_layer(state):
        x = jnp.concatenate(state, axis=1)
        return split(apply_rows(apply_lanes(x, lane1), home1) * sign2)

    inside = [(q, s) for q, s in zip(local, spots) if q not in (0, 14)]
    tally(0, [q for q, _ in inside], home_terms(home_layer(bra), home_layer(ket), [s for _, s in inside]))

    def give_sums():
        lane8 = lax.broadcasted_iota(jnp.int32, (8, 128), 1)
        mine = jnp.zeros((8, 128), F32)
        for layer in range(2):
            for k in range(3):
                value = 0.5 * jnp.sum(acc[layer, k], keepdims=True)
                mine = mine + jnp.where(lane8 == 3 * layer + k, value, 0.0)
        part[...] = mine
        from_plane[pl.ds(plane, 1)] = mine[None]

        def hand_over(d, spot):
            pltpu.make_async_remote_copy(
                src_ref=part, dst_ref=from_plane.at[plane], send_sem=send_sems.at[4], recv_sem=recv_sems.at[4],
                device_id=(d,), device_id_type=MESH,
            ).start()

        to_plane(hand_over)

    row_spots = [(0, p) for p in range(8)]

    def visit(chunk, arrived, source, send, recv, slot):
        start_sign = entangle(me, ALL_PAIRS, chunk)
        away_sign = entangle(me, AWAY_PAIRS, chunk)
        arrived.wait_recv()
        obs = recv_a[1]
        keep = lane_bit4()
        obs = jnp.where(keep, obs, up(obs)) if chunk == 0 else jnp.where(keep, down(obs), obs)
        ket = source[0] * start_sign
        bra = obs * scale * ket

        def away_layer(x):
            x = mm(cut(x), (chunk_lane1[0], chunk_lane1[1]))
            return apply_chunk_rows(x, away1) * away_sign

        def leave(bra_x):
            send[0] = apply_chunk_rows(bra_x, away0)
            keep_own(send, recv)
            exchange(send, recv, slot)

        def take_terms(bra_x, ket_x):
            tally(1, AWAY_ROWS, chunk_terms(bra, ket, row_spots))
            tally(0, list(AWAY_ROWS) + [0, 14], chunk_terms(bra_x, ket_x, row_spots + [(1, 0), (1, 6)]))

        if chunk == 0:
            bra_x = away_layer(bra)
            leave(bra_x)
            take_terms(bra_x, away_layer(ket))
        else:
            x = jnp.concatenate([bra, ket], axis=0)
            x = mm(cut(x), (chunk_lane1[0], chunk_lane1[1]))
            x = cut(jnp.concatenate([x[:256], x[256:]], axis=1))
            a, b = mm((away1[0, 0], away1[0, 1]), x), mm((away1[1, 0], away1[1, 1]), x)
            bra_x = (a[:, :128] + times_i(b[:, :128])) * away_sign
            ket_x = (a[:, 128:] + times_i(b[:, 128:])) * away_sign
            take_terms(bra_x, ket_x)
            give_sums()
            leave(bra_x)

    visit(0, out_a, recv_a, send_c, recv_c, 2)
    out_c = exchanged(send_c, recv_c, 2)
    visit(1, out_b, recv_b, send_d, recv_d, 3)
    out_d = exchanged(send_d, recv_d, 3)

    third = pltpu.make_async_remote_copy(
        src_ref=from_plane.at[pl.ds(0, 31)], dst_ref=from_plane.at[pl.ds(0, 31)],
        send_sem=send_sems.at[4], recv_sem=recv_sems.at[4], device_id=(me,), device_id_type=MESH,
    )
    build_lane(lane0, 0)
    build_rows(home0, 0, HOME_ROWS)
    rest_sign = entangle(me, REST_PAIRS)
    rest2 = jnp.concatenate([rest_sign, rest_sign], axis=1)

    third.wait_recv()
    summed = jnp.sum(from_plane[...], axis=0)
    part_z[...] = summed
    from_z[pl.ds(z, 1)] = summed[None]
    for dz in (4, 3, 5, 2, 6, 1, 7):
        pltpu.make_async_remote_copy(
            src_ref=part_z, dst_ref=from_z.at[z], send_sem=send_sems.at[5], recv_sem=recv_sems.at[5],
            device_id=(((z + dz) % 8) * 32 + plane,), device_id_type=MESH,
        ).start()
    fourth = pltpu.make_async_remote_copy(
        src_ref=from_z.at[pl.ds(0, 7)], dst_ref=from_z.at[pl.ds(0, 7)],
        send_sem=send_sems.at[5], recv_sem=recv_sems.at[5], device_id=(me,), device_id_type=MESH,
    )

    cosine, sy, sz = coefs(1, 4)
    out_c.wait_recv()
    low = apply_chunk_rows(recv_c[0], home1)
    out_d.wait_recv()
    high = apply_chunk_rows(recv_d[0], home1)
    low, high = (
        cosine * low + sy * high + sz * times_i(low),
        cosine * high - sy * low - sz * times_i(high),
    )
    x2 = jnp.concatenate(from_chunks(low, high), axis=1) * rest2
    x2 = apply_rows(apply_lanes(x2, lane0), home0)
    bra_ref[0], bra_ref[1] = split(x2)

    fourth.wait_recv()
    grads_ref[...] = jnp.sum(from_z[...], axis=0)
    for copy in (out_a, out_b, out_c, out_d, third, fourth):
        copy.wait_send()


def finish(state, sums, bra_hbm, grads_ref, raw, out_sem):
    stores = []
    for i in range(2):
        raw[i] = repack(state[i])
        stores.append(pltpu.make_async_copy(raw.at[i], bra_hbm.at[:, i, :], out_sem.at[i]))
        stores[i].start()
    total = sums[0:1, :]
    grads_ref[...] = jnp.concatenate([total[:, 0:3], total[:, 3:6]], axis=0)
    for copy in stores:
        copy.wait()


def on_device(ket_state, observable, angles, gate_kinds):
    ket = ket_state.reshape(2, 256, 128).transpose(1, 0, 2)
    obs = observable.reshape(256, 128)
    main_memory = pl.BlockSpec(memory_space=pltpu.HBM)
    vmem = lambda *shape, dtype=F32: pltpu.VMEM(shape, dtype)
    half = lambda *shape: pltpu.VMEM(shape, jnp.bfloat16)
    on_chip = pl.BlockSpec(memory_space=pltpu.VMEM)
    state, sums = pl.pallas_call(
        kernel,
        out_shape=(
            jax.ShapeDtypeStruct((2, 256, 128), F32),
            jax.ShapeDtypeStruct((8, 128), F32),
        ),
        in_specs=[main_memory] * 4,
        out_specs=(on_chip, on_chip),
        scratch_shapes=[
            pltpu.SMEM((2, 3), F32), pltpu.SMEM((2, 32), jnp.int32),
            vmem(3, 256, 128),
            vmem(2, 256, 128), vmem(1, 256, 128), vmem(2, 256, 128), vmem(1, 256, 128),
            vmem(1, 256, 128), vmem(1, 256, 128), vmem(1, 256, 128), vmem(1, 256, 128),
            vmem(48, 128), vmem(48, 128, dtype=jnp.int32),
            vmem(48, 128), vmem(48, 128), vmem(48, 128),
            half(2, 256, 256), half(2, 256, 256), half(2, 128, 128),
            half(2, 2, 256, 256), half(2, 2, 256, 256), half(2, 2, 256, 256), half(2, 2, 256, 256),
            vmem(8, 128), vmem(8, 8, 128), vmem(8, 128), vmem(32, 8, 128),
            pltpu.SemaphoreType.DMA((5,)),
            pltpu.SemaphoreType.DMA((6,)), pltpu.SemaphoreType.DMA((6,)),
        ],
        compiler_params=pltpu.CompilerParams(
            collective_id=0, has_side_effects=True, vmem_limit_bytes=16 << 20
        ),
    )(*(pltpu.with_memory_space_constraint(v, pltpu.HBM) for v in (ket, obs, angles, gate_kinds)))
    bra, grads = pl.pallas_call(
        finish,
        out_shape=(
            jax.ShapeDtypeStruct((256, 2, 128), F32),
            jax.ShapeDtypeStruct((2, 3), F32),
        ),
        in_specs=[on_chip, on_chip],
        out_specs=(main_memory, on_chip),
        scratch_shapes=[vmem(2, 256, 128), pltpu.SemaphoreType.DMA((2,))],
        compiler_params=pltpu.CompilerParams(vmem_limit_bytes=4 << 20),
    )(state, sums)
    return bra.transpose(1, 0, 2).reshape(2, 32768), grads


def solution(mesh):
    return jax.shard_map(
        on_device,
        mesh=mesh,
        in_specs=(P(None, "amp"), P("amp"), P(), P()),
        out_specs=(P(None, "amp"), P()),
        check_vma=False,
    )
```

```python
import functools
import math

import jax
import jax.numpy as jnp
from jax import lax
from jax.experimental import pallas as pl
from jax.experimental.pallas import tpu as pltpu
from jax.sharding import PartitionSpec as P

MESH = pl.DeviceIdType.MESH
QUBITS = 23
LANE_QUBITS = (0, 1, 2, 3, 4, 13, 14)
HOME_ROWS = (7, 8, 9, 10, 11, 12, 5, 6)
AWAY_ROWS = (15, 16, 17, 18, 19, 20, 21, 22)
F32 = jnp.float32


def pair_mask(qubits):
    return sum(1 << q for q in qubits)


ALL_PAIRS = pair_mask(range(QUBITS))
LOCAL_PAIRS = pair_mask(range(14))
AWAY_PAIRS = pair_mask([0] + list(range(13, 23)))
REST_PAIRS = ALL_PAIRS - AWAY_PAIRS


def row_lane():
    row = lax.broadcasted_iota(jnp.int32, (256, 128), 0)
    lane = lax.broadcasted_iota(jnp.int32, (256, 128), 1)
    return row, lane


def entangle(me, pairs, chunk=None):
    row, lane = row_lane()
    own = me + jnp.zeros_like(row)
    far, near = (own, row) if chunk is None else (row, own)
    low = lane & 31 if chunk is None else (lane & 15) | (chunk << 4)
    index = low | ((near >> 6) << 5) | ((near & 63) << 7) | ((lane >> 5) << 13) | (far << 15)
    both = index & ((index >> 1) | ((index & 1) << 22)) & pairs
    for shift in (16, 8, 4, 2, 1):
        both = both ^ (both >> shift)
    return (1 - 2 * (both & 1)).astype(F32)


def swap_bits(x, row_bit, lane_bit):
    rows = 1 << row_bit
    parts = x.reshape(256 // (2 * rows), 2, rows, 128)
    low, high = parts[:, 0].reshape(128, 128), parts[:, 1].reshape(128, 128)
    step = 1 << lane_bit
    lane = lax.broadcasted_iota(jnp.int32, (128, 128), 1)
    keep = (lane & step) == 0
    new_low = jnp.where(keep, low, pltpu.roll(high, step, 1))
    new_high = jnp.where(keep, pltpu.roll(low, 128 - step, 1), high)
    shape = (256 // (2 * rows), 1, rows, 128)
    return jnp.concatenate([new_low.reshape(shape), new_high.reshape(shape)], axis=1).reshape(256, 128)


def repack(x):
    return swap_bits(swap_bits(x, 6, 5), 7, 6)


def lane_bit4():
    return (lax.broadcasted_iota(jnp.int32, (256, 128), 1) & 16) == 0


def up(x):
    return pltpu.roll(x, 16, 1)


def down(x):
    return pltpu.roll(x, 112, 1)


def to_chunks(real, imag):
    keep = lane_bit4()
    return jnp.where(keep, real, up(imag)), jnp.where(keep, down(real), imag)


def from_chunks(first, second):
    keep = lane_bit4()
    return jnp.where(keep, first, up(second)), jnp.where(keep, down(first), second)


def times_i(x):
    return jnp.where(lane_bit4(), -down(x), up(x))


def fold8(x):
    return jnp.sum(x.reshape(-1, 8, 128), axis=0)


def bit_sign(axis, position):
    place = lax.broadcasted_iota(jnp.int32, (8, 128), axis)
    return (1 - 2 * ((place >> position) & 1)).astype(F32)


def halves(x, position):
    parts = x.reshape(256 >> (position + 1), 2, 1 << position, 128)
    return parts[:, 0], parts[:, 1]


def flip(x, axis, position):
    step = 1 << position
    if axis == 0:
        y = x.reshape(32, 8, 128)
        place = lax.broadcasted_iota(jnp.int32, (32, 8, 128), 1)
        up, down = pltpu.roll(y, 8 - step, 1), pltpu.roll(y, step, 1)
        return jnp.where((place & step) == 0, up, down).reshape(256, 128)
    place = lax.broadcasted_iota(jnp.int32, (256, 128), 1)
    return jnp.where((place & step) == 0, pltpu.roll(x, 128 - step, 1), pltpu.roll(x, step, 1))


def terms(bras, kets, cross, spots):
    total = fold8(cross)
    out = []
    for axis, position in spots:
        if axis == 0 and position >= 3:
            y_part = 0.0
            for bra, ket in zip(bras, kets):
                b0, b1 = halves(bra, position)
                k0, k1 = halves(ket, position)
                y_part = y_part + (b1 * k0 - b0 * k1)
            y_part = fold8(y_part)
            c0, c1 = halves(cross, position)
            z_part = fold8(c0 - c1)
        else:
            sign = bit_sign(axis, position)
            pairs = sum(bra * flip(ket, axis, position) for bra, ket in zip(bras, kets))
            y_part = -sign * fold8(pairs)
            z_part = sign * total
        out.append((y_part, z_part))
    return out


def chunk_terms(bra, ket, spots):
    turned = flip(ket, 1, 4)
    cross = bra * jnp.where(lane_bit4(), turned, -turned)
    return terms([bra], [ket], cross, spots)


def home_terms(bra, ket, spots):
    return terms(bra, ket, bra[0] * ket[1] - bra[1] * ket[0], spots)


def cut(x):
    high = x.astype(jnp.bfloat16)
    return high, (x - high.astype(F32)).astype(jnp.bfloat16)


def mm(a, b):
    (a_high, a_low), (b_high, b_low) = a, b
    dot = functools.partial(jnp.dot, preferred_element_type=F32)
    return dot(a_high, b_high) + (dot(a_high, b_low) + dot(a_low, b_high))


def kernel(
    ket_hbm, obs_hbm, angles_hbm, kinds_hbm,
    bra_ref, grads_ref,
    angles, kinds, raw, send_a, send_b, recv_a, recv_b, send_c, send_d, recv_c, recv_d,
    theta, kind_tab, cos_tab, sy_tab, sz_tab,
    lane1, lane0, chunk_lane1, home1, home0, away1, away0,
    part, from_z, part_z, from_plane,
    in_sem, send_sems, recv_sems,
):
    me = lax.axis_index("amp")
    z, y, x, c = me // 32, (me // 8) % 4, (me // 2) % 4, me % 2
    plane = me % 32
    inner = [((x + dx) % 4) * 2 + (c + dc) % 2 for dx in (2, 1, 3, 0) for dc in (0, 1)]
    tiers = [((y + dy) % 4) * 8 for dy in (2, 1, 3, 0)]

    def to_all(act):
        def body(step, carry):
            dz = jnp.where(step % 2 == 0, 4 + step // 2, 4 - (step + 1) // 2)
            base = ((z + dz) % 8) * 32
            for tier in tiers:
                for spot in inner:
                    act(base + tier + spot)
            return carry

        lax.fori_loop(0, 7, body, 0)
        to_plane(lambda d, spot: act(d))

    def to_plane(act):
        for t, tier in enumerate(tiers):
            for s, spot in enumerate(inner):
                if (t, s) != (3, 6):
                    act(z * 32 + tier + spot, tier + spot)

    barrier = pltpu.get_barrier_semaphore()
    to_all(lambda d: pl.semaphore_signal(barrier, inc=1, device_id=(d,), device_id_type=MESH))

    loads = [
        pltpu.make_async_copy(ket_hbm.at[:, 0, :], raw.at[0], in_sem.at[0]),
        pltpu.make_async_copy(ket_hbm.at[:, 1, :], raw.at[1], in_sem.at[1]),
        pltpu.make_async_copy(obs_hbm, raw.at[2], in_sem.at[2]),
    ]
    settings = [
        pltpu.make_async_copy(angles_hbm, angles, in_sem.at[3]),
        pltpu.make_async_copy(kinds_hbm, kinds, in_sem.at[4]),
    ]
    for copy in loads + settings:
        copy.start()

    def coefs(layer, q):
        row = slice(layer * 24 + q, layer * 24 + q + 1)
        return cos_tab[row, :], sy_tab[row, :], sz_tab[row, :]

    def kron(value, out_bits, in_bits, layer, qubits):
        real, imag = value
        for position, q in qubits:
            cosine, sy, sz = coefs(layer, q)
            if out_bits.shape[1] > 128:
                cosine, sy, sz = (jnp.concatenate([v, v], axis=1) for v in (cosine, sy, sz))
            b_out = (out_bits >> position) & 1
            b_in = (in_bits >> position) & 1
            same = b_out == b_in
            a = jnp.where(same, cosine, sy * (b_in - b_out).astype(F32))
            b = jnp.where(same, sz * (1 - 2 * b_out).astype(F32), 0.0)
            if real is None:
                real, imag = a, b
            else:
                real, imag = real * a - imag * b, real * b + imag * a
        return real, imag

    def build_lane(ref, layer):
        j = lax.broadcasted_iota(jnp.int32, (128, 128), 0)
        k = lax.broadcasted_iota(jnp.int32, (128, 128), 1)
        real, imag = kron((None, None), k, j, layer, list(enumerate(LANE_QUBITS)))
        for i, (re, im) in enumerate(zip(cut(real), cut(imag))):
            ref[i, 0:128, 0:128] = re
            ref[i, 128:256, 128:256] = re
            ref[i, 0:128, 128:256] = im
            ref[i, 128:256, 0:128] = -im

    def build_chunk_lane(ref, layer):
        j = lax.broadcasted_iota(jnp.int32, (128, 128), 0)
        k = lax.broadcasted_iota(jnp.int32, (128, 128), 1)
        qubits = [(p, q) for p, q in enumerate(LANE_QUBITS) if p != 4]
        real, imag = kron((None, None), k, j, layer, qubits)
        part_in, part_out = (j >> 4) & 1, (k >> 4) & 1
        mixed = jnp.where(part_in == part_out, real, jnp.where(part_out == 1, imag, -imag))
        ref[0], ref[1] = cut(mixed)

    def build_rows(ref, layer, qubits):
        places = list(enumerate(qubits))
        j = lax.broadcasted_iota(jnp.int32, (32, 256), 0)
        k = lax.broadcasted_iota(jnp.int32, (32, 256), 1)
        base = kron((None, None), j, k, layer, places[:5])

        def body(block, carry):
            real, imag = kron(base, j + block * 32, k, layer, places[5:])
            at = pl.ds(pl.multiple_of(block * 32, 32), 32)
            for i, (re, im) in enumerate(zip(cut(real), cut(imag))):
                ref[0, i, at, :] = re
                ref[1, i, at, :] = im
            return carry

        lax.fori_loop(0, 8, body, 0)

    def apply_lanes(x, ref):
        return mm(cut(x), (ref[0], ref[1]))

    def apply_rows(x, ref):
        x = cut(x)
        a, b = mm((ref[0, 0], ref[0, 1]), x), mm((ref[1, 0], ref[1, 1]), x)
        return jnp.concatenate([a[:, :128] - b[:, 128:], a[:, 128:] + b[:, :128]], axis=1)

    def apply_chunk_rows(x, ref):
        x = cut(x)
        return mm((ref[0, 0], ref[0, 1]), x) + times_i(mm((ref[1, 0], ref[1, 1]), x))

    def split(x):
        return x[:, :128], x[:, 128:]

    for copy in loads:
        copy.wait()
    for i in range(3):
        raw[i] = repack(raw[i])
    send_a[0], send_b[0] = to_chunks(raw[0], raw[1])
    send_a[1] = raw[2]

    def keep_own(source, target):
        target[:, pl.ds(me, 1), :] = source[:, pl.ds(me, 1), :]

    keep_own(send_a, recv_a)
    keep_own(send_b, recv_b)

    pl.semaphore_wait(barrier, 255)

    def exchange(source, target, slot):
        def act(d):
            pltpu.make_async_remote_copy(
                src_ref=source.at[:, pl.ds(d, 1), :],
                dst_ref=target.at[:, pl.ds(me, 1), :],
                send_sem=send_sems.at[slot],
                recv_sem=recv_sems.at[slot],
                device_id=(d,),
                device_id_type=MESH,
            ).start()

        to_all(act)

    def exchanged(source, target, slot):
        return pltpu.make_async_remote_copy(
            src_ref=source.at[:, pl.ds(0, 255), :],
            dst_ref=target.at[:, pl.ds(0, 255), :],
            send_sem=send_sems.at[slot],
            recv_sem=recv_sems.at[slot],
            device_id=(me,),
            device_id_type=MESH,
        )

    exchange(send_a, recv_a, 0)
    exchange(send_b, recv_b, 1)
    out_a = exchanged(send_a, recv_a, 0)
    out_b = exchanged(send_b, recv_b, 1)

    for copy in settings:
        copy.wait()
    theta[...] = jnp.zeros_like(theta)
    kind_tab[...] = jnp.zeros_like(kind_tab)
    picks = {}
    for layer in range(2):
        for q in range(QUBITS):
            kind = kinds[layer, q]
            picks[layer, q] = [jnp.where(kind == k, 1.0, 0.0).astype(F32) for k in range(3)]
            angle = jnp.where(
                kind == 0, angles[layer, 0], jnp.where(kind == 1, angles[layer, 1], angles[layer, 2])
            )
            row = layer * 24 + q
            theta[row : row + 1, :] = jnp.full((1, 128), 0.5 * angle, F32)
            kind_tab[row : row + 1, :] = jnp.full((1, 128), kind, jnp.int32)
    cos_tab[...] = jnp.cos(theta[...])
    sines = jnp.sin(theta[...])
    is_z = kind_tab[...] == 2
    sy_tab[...] = jnp.where(is_z, 0.0, sines)
    sz_tab[...] = jnp.where(is_z, sines, 0.0)

    build_chunk_lane(chunk_lane1, 1)
    build_rows(away1, 1, AWAY_ROWS)
    build_rows(away0, 0, AWAY_ROWS)
    build_lane(lane1, 1)
    build_rows(home1, 1, HOME_ROWS)

    scale = 2.0 / math.sqrt(1 << QUBITS)

    acc = {(layer, k): jnp.zeros((8, 128), F32) for layer in range(2) for k in range(3)}

    def tally(layer, qubits, values):
        for q, (y_part, z_part) in zip(qubits, values):
            pick = picks[layer, q]
            acc[layer, 0] = acc[layer, 0] + pick[0] * y_part
            acc[layer, 1] = acc[layer, 1] + pick[1] * y_part
            acc[layer, 2] = acc[layer, 2] + pick[2] * z_part

    spots = [(1, p) for p in range(7)] + [(0, p) for p in range(8)]
    local = list(LANE_QUBITS) + list(HOME_ROWS)
    sign = entangle(me, ALL_PAIRS)
    ket = (raw[0] * sign, raw[1] * sign)
    bra = tuple(raw[2] * scale * part for part in ket)
    tally(1, local, home_terms(bra, ket, spots))
    local_sign = entangle(me, LOCAL_PAIRS)
    sign2 = jnp.concatenate([local_sign, local_sign], axis=1)

    def home_layer(state):
        x = jnp.concatenate(state, axis=1)
        return split(apply_rows(apply_lanes(x, lane1), home1) * sign2)

    inside = [(q, s) for q, s in zip(local, spots) if q not in (0, 14)]
    tally(0, [q for q, _ in inside], home_terms(home_layer(bra), home_layer(ket), [s for _, s in inside]))

    def give_sums():
        lane8 = lax.broadcasted_iota(jnp.int32, (8, 128), 1)
        mine = jnp.zeros((8, 128), F32)
        for layer in range(2):
            for k in range(3):
                value = 0.5 * jnp.sum(acc[layer, k], keepdims=True)
                mine = mine + jnp.where(lane8 == 3 * layer + k, value, 0.0)
        part[...] = mine
        from_plane[pl.ds(plane, 1)] = mine[None]

        def hand_over(d, spot):
            pltpu.make_async_remote_copy(
                src_ref=part, dst_ref=from_plane.at[plane], send_sem=send_sems.at[4], recv_sem=recv_sems.at[4],
                device_id=(d,), device_id_type=MESH,
            ).start()

        to_plane(hand_over)

    row_spots = [(0, p) for p in range(8)]

    def visit(chunk, arrived, source, send, recv, slot):
        start_sign = entangle(me, ALL_PAIRS, chunk)
        away_sign = entangle(me, AWAY_PAIRS, chunk)
        arrived.wait_recv()
        obs = recv_a[1]
        keep = lane_bit4()
        obs = jnp.where(keep, obs, up(obs)) if chunk == 0 else jnp.where(keep, down(obs), obs)
        ket = source[0] * start_sign
        bra = obs * scale * ket

        def away_layer(x):
            x = mm(cut(x), (chunk_lane1[0], chunk_lane1[1]))
            return apply_chunk_rows(x, away1) * away_sign

        def leave(bra_x):
            send[0] = apply_chunk_rows(bra_x, away0)
            keep_own(send, recv)
            exchange(send, recv, slot)

        def take_terms(bra_x, ket_x):
            tally(1, AWAY_ROWS, chunk_terms(bra, ket, row_spots))
            tally(0, list(AWAY_ROWS) + [0, 14], chunk_terms(bra_x, ket_x, row_spots + [(1, 0), (1, 6)]))

        if chunk == 0:
            bra_x = away_layer(bra)
            leave(bra_x)
            take_terms(bra_x, away_layer(ket))
        else:
            x = jnp.concatenate([bra, ket], axis=0)
            x = mm(cut(x), (chunk_lane1[0], chunk_lane1[1]))
            x = cut(jnp.concatenate([x[:256], x[256:]], axis=1))
            a, b = mm((away1[0, 0], away1[0, 1]), x), mm((away1[1, 0], away1[1, 1]), x)
            bra_x = (a[:, :128] + times_i(b[:, :128])) * away_sign
            ket_x = (a[:, 128:] + times_i(b[:, 128:])) * away_sign
            take_terms(bra_x, ket_x)
            give_sums()
            leave(bra_x)

    visit(0, out_a, recv_a, send_c, recv_c, 2)
    out_c = exchanged(send_c, recv_c, 2)
    visit(1, out_b, recv_b, send_d, recv_d, 3)
    out_d = exchanged(send_d, recv_d, 3)

    third = pltpu.make_async_remote_copy(
        src_ref=from_plane.at[pl.ds(0, 31)], dst_ref=from_plane.at[pl.ds(0, 31)],
        send_sem=send_sems.at[4], recv_sem=recv_sems.at[4], device_id=(me,), device_id_type=MESH,
    )
    build_lane(lane0, 0)
    build_rows(home0, 0, HOME_ROWS)
    rest_sign = entangle(me, REST_PAIRS)
    rest2 = jnp.concatenate([rest_sign, rest_sign], axis=1)

    third.wait_recv()
    summed = jnp.sum(from_plane[...], axis=0)
    part_z[...] = summed
    from_z[pl.ds(z, 1)] = summed[None]
    for dz in (4, 3, 5, 2, 6, 1, 7):
        pltpu.make_async_remote_copy(
            src_ref=part_z, dst_ref=from_z.at[z], send_sem=send_sems.at[5], recv_sem=recv_sems.at[5],
            device_id=(((z + dz) % 8) * 32 + plane,), device_id_type=MESH,
        ).start()
    fourth = pltpu.make_async_remote_copy(
        src_ref=from_z.at[pl.ds(0, 7)], dst_ref=from_z.at[pl.ds(0, 7)],
        send_sem=send_sems.at[5], recv_sem=recv_sems.at[5], device_id=(me,), device_id_type=MESH,
    )

    cosine, sy, sz = coefs(1, 4)
    out_c.wait_recv()
    low = apply_chunk_rows(recv_c[0], home1)
    out_d.wait_recv()
    high = apply_chunk_rows(recv_d[0], home1)
    low, high = (
        cosine * low + sy * high + sz * times_i(low),
        cosine * high - sy * low - sz * times_i(high),
    )
    x2 = jnp.concatenate(from_chunks(low, high), axis=1) * rest2
    x2 = apply_rows(apply_lanes(x2, lane0), home0)
    bra_ref[0], bra_ref[1] = split(x2)

    fourth.wait_recv()
    grads_ref[...] = jnp.sum(from_z[...], axis=0)
    for copy in (out_a, out_b, out_c, out_d, third, fourth):
        copy.wait_send()


def finish(state, sums, bra_hbm, grads_ref, raw, out_sem):
    for i in range(2):
        raw[pl.ds(i, 256, 2), :] = repack(state[i])
    store = pltpu.make_async_copy(raw, bra_hbm, out_sem)
    store.start()
    total = sums[0:1, :]
    grads_ref[...] = jnp.concatenate([total[:, 0:3], total[:, 3:6]], axis=0)
    store.wait()


def on_device(ket_state, observable, angles, gate_kinds):
    ket = ket_state.reshape(2, 256, 128).transpose(1, 0, 2)
    obs = observable.reshape(256, 128)
    main_memory = pl.BlockSpec(memory_space=pltpu.HBM)
    vmem = lambda *shape, dtype=F32: pltpu.VMEM(shape, dtype)
    half = lambda *shape: pltpu.VMEM(shape, jnp.bfloat16)
    on_chip = pl.BlockSpec(memory_space=pltpu.VMEM)
    state, sums = pl.pallas_call(
        kernel,
        out_shape=(
            jax.ShapeDtypeStruct((2, 256, 128), F32),
            jax.ShapeDtypeStruct((8, 128), F32),
        ),
        in_specs=[main_memory] * 4,
        out_specs=(on_chip, on_chip),
        scratch_shapes=[
            pltpu.SMEM((2, 3), F32), pltpu.SMEM((2, 32), jnp.int32),
            vmem(3, 256, 128),
            vmem(2, 256, 128), vmem(1, 256, 128), vmem(2, 256, 128), vmem(1, 256, 128),
            vmem(1, 256, 128), vmem(1, 256, 128), vmem(1, 256, 128), vmem(1, 256, 128),
            vmem(48, 128), vmem(48, 128, dtype=jnp.int32),
            vmem(48, 128), vmem(48, 128), vmem(48, 128),
            half(2, 256, 256), half(2, 256, 256), half(2, 128, 128),
            half(2, 2, 256, 256), half(2, 2, 256, 256), half(2, 2, 256, 256), half(2, 2, 256, 256),
            vmem(8, 128), vmem(8, 8, 128), vmem(8, 128), vmem(32, 8, 128),
            pltpu.SemaphoreType.DMA((5,)),
            pltpu.SemaphoreType.DMA((6,)), pltpu.SemaphoreType.DMA((6,)),
        ],
        compiler_params=pltpu.CompilerParams(
            collective_id=0, has_side_effects=True, vmem_limit_bytes=16 << 20
        ),
    )(*(pltpu.with_memory_space_constraint(v, pltpu.HBM) for v in (ket, obs, angles, gate_kinds)))
    bra, grads = pl.pallas_call(
        finish,
        out_shape=(
            jax.ShapeDtypeStruct((512, 128), F32),
            jax.ShapeDtypeStruct((2, 3), F32),
        ),
        in_specs=[on_chip, on_chip],
        out_specs=(main_memory, on_chip),
        scratch_shapes=[vmem(512, 128), pltpu.SemaphoreType.DMA(())],
        compiler_params=pltpu.CompilerParams(vmem_limit_bytes=4 << 20),
    )(state, sums)
    return bra.reshape(256, 2, 128).transpose(1, 0, 2).reshape(2, 32768), grads


def solution(mesh):
    return jax.shard_map(
        on_device,
        mesh=mesh,
        in_specs=(P(None, "amp"), P("amp"), P(), P()),
        out_specs=(P(None, "amp"), P()),
        check_vma=False,
    )
```

```python
import functools
import math

import jax
import jax.numpy as jnp
from jax import lax
from jax.experimental import pallas as pl
from jax.experimental.pallas import tpu as pltpu
from jax.sharding import PartitionSpec as P

MESH = pl.DeviceIdType.MESH
QUBITS = 23
LANE_QUBITS = (0, 1, 2, 3, 4, 13, 14)
HOME_ROWS = (7, 8, 9, 10, 11, 12, 5, 6)
AWAY_ROWS = (15, 16, 17, 18, 19, 20, 21, 22)
F32 = jnp.float32


def pair_mask(qubits):
    return sum(1 << q for q in qubits)


ALL_PAIRS = pair_mask(range(QUBITS))
LOCAL_PAIRS = pair_mask(range(14))
AWAY_PAIRS = pair_mask([0] + list(range(13, 23)))
REST_PAIRS = ALL_PAIRS - AWAY_PAIRS


def row_lane():
    row = lax.broadcasted_iota(jnp.int32, (256, 128), 0)
    lane = lax.broadcasted_iota(jnp.int32, (256, 128), 1)
    return row, lane


def entangle(me, pairs, chunk=None):
    row, lane = row_lane()
    own = me + jnp.zeros_like(row)
    far, near = (own, row) if chunk is None else (row, own)
    low = lane & 31 if chunk is None else (lane & 15) | (chunk << 4)
    index = low | ((near >> 6) << 5) | ((near & 63) << 7) | ((lane >> 5) << 13) | (far << 15)
    both = index & ((index >> 1) | ((index & 1) << 22)) & pairs
    for shift in (16, 8, 4, 2, 1):
        both = both ^ (both >> shift)
    return (1 - 2 * (both & 1)).astype(F32)


def swap_bits(x, row_bit, lane_bit):
    rows = 1 << row_bit
    parts = x.reshape(256 // (2 * rows), 2, rows, 128)
    low, high = parts[:, 0].reshape(128, 128), parts[:, 1].reshape(128, 128)
    step = 1 << lane_bit
    lane = lax.broadcasted_iota(jnp.int32, (128, 128), 1)
    keep = (lane & step) == 0
    new_low = jnp.where(keep, low, pltpu.roll(high, step, 1))
    new_high = jnp.where(keep, pltpu.roll(low, 128 - step, 1), high)
    shape = (256 // (2 * rows), 1, rows, 128)
    return jnp.concatenate([new_low.reshape(shape), new_high.reshape(shape)], axis=1).reshape(256, 128)


def repack(x):
    return swap_bits(swap_bits(x, 6, 5), 7, 6)


def lane_bit4():
    return (lax.broadcasted_iota(jnp.int32, (256, 128), 1) & 16) == 0


def up(x):
    return pltpu.roll(x, 16, 1)


def down(x):
    return pltpu.roll(x, 112, 1)


def to_chunks(real, imag):
    keep = lane_bit4()
    return jnp.where(keep, real, up(imag)), jnp.where(keep, down(real), imag)


def from_chunks(first, second):
    keep = lane_bit4()
    return jnp.where(keep, first, up(second)), jnp.where(keep, down(first), second)


def times_i(x):
    return jnp.where(lane_bit4(), -down(x), up(x))


def fold8(x):
    return jnp.sum(x.reshape(-1, 8, 128), axis=0)


def bit_sign(axis, position):
    place = lax.broadcasted_iota(jnp.int32, (8, 128), axis)
    return (1 - 2 * ((place >> position) & 1)).astype(F32)


def halves(x, position):
    parts = x.reshape(256 >> (position + 1), 2, 1 << position, 128)
    return parts[:, 0], parts[:, 1]


def flip(x, axis, position):
    step = 1 << position
    if axis == 0:
        y = x.reshape(32, 8, 128)
        place = lax.broadcasted_iota(jnp.int32, (32, 8, 128), 1)
        up, down = pltpu.roll(y, 8 - step, 1), pltpu.roll(y, step, 1)
        return jnp.where((place & step) == 0, up, down).reshape(256, 128)
    place = lax.broadcasted_iota(jnp.int32, (256, 128), 1)
    return jnp.where((place & step) == 0, pltpu.roll(x, 128 - step, 1), pltpu.roll(x, step, 1))


def terms(bras, kets, cross, spots):
    total = fold8(cross)
    out = []
    for axis, position in spots:
        if axis == 0 and position >= 3:
            y_part = 0.0
            for bra, ket in zip(bras, kets):
                b0, b1 = halves(bra, position)
                k0, k1 = halves(ket, position)
                y_part = y_part + (b1 * k0 - b0 * k1)
            y_part = fold8(y_part)
            c0, c1 = halves(cross, position)
            z_part = fold8(c0 - c1)
        else:
            sign = bit_sign(axis, position)
            pairs = sum(bra * flip(ket, axis, position) for bra, ket in zip(bras, kets))
            y_part = -sign * fold8(pairs)
            z_part = sign * total
        out.append((y_part, z_part))
    return out


def chunk_terms(bra, ket, spots):
    turned = flip(ket, 1, 4)
    cross = bra * jnp.where(lane_bit4(), turned, -turned)
    return terms([bra], [ket], cross, spots)


def home_terms(bra, ket, spots):
    return terms(bra, ket, bra[0] * ket[1] - bra[1] * ket[0], spots)


def cut(x):
    high = x.astype(jnp.bfloat16)
    return high, (x - high.astype(F32)).astype(jnp.bfloat16)


def mm(a, b):
    (a_high, a_low), (b_high, b_low) = a, b
    dot = functools.partial(jnp.dot, preferred_element_type=F32)
    return dot(a_high, b_high) + (dot(a_high, b_low) + dot(a_low, b_high))


def kernel(
    ket_hbm, obs_hbm, angles_hbm, kinds_hbm,
    bra_ref, grads_ref,
    angles, kinds, raw, send_a, send_b, recv_a, recv_b, send_c, send_d, recv_c, recv_d,
    theta, kind_tab, cos_tab, sy_tab, sz_tab,
    lane1, lane0, chunk_lane1, home1, home0, away1, away0,
    part, from_z, part_z, from_plane,
    in_sem, send_sems, recv_sems,
):
    me = lax.axis_index("amp")
    z, y, x, c = me // 32, (me // 8) % 4, (me // 2) % 4, me % 2
    plane = me % 32
    inner = [((x + dx) % 4) * 2 + (c + dc) % 2 for dx in (2, 1, 3, 0) for dc in (0, 1)]
    tiers = [((y + dy) % 4) * 8 for dy in (2, 1, 3, 0)]

    columns = [((z + dz) % 8) * 32 for dz in (4, 3, 5, 2, 6, 1, 7, 0)]

    def to_all(act):
        def body(step, carry):
            dy, dx, dc = step // 8 + 2, (step // 2) % 4 + 2, step % 2
            spot = ((y + dy) % 4) * 8 + ((x + dx) % 4) * 2 + (c + dc) % 2
            for column in columns:
                act(column + spot)
            return carry

        lax.fori_loop(0, 20, body, 0)
        lax.fori_loop(21, 32, body, 0)
        for column in columns[:7]:
            act(column + plane)

    def to_plane(act):
        for t, tier in enumerate(tiers):
            for s, spot in enumerate(inner):
                if (t, s) != (3, 6):
                    act(z * 32 + tier + spot, tier + spot)

    barrier = pltpu.get_barrier_semaphore()
    to_all(lambda d: pl.semaphore_signal(barrier, inc=1, device_id=(d,), device_id_type=MESH))

    loads = [
        pltpu.make_async_copy(ket_hbm.at[:, 0, :], raw.at[0], in_sem.at[0]),
        pltpu.make_async_copy(ket_hbm.at[:, 1, :], raw.at[1], in_sem.at[1]),
        pltpu.make_async_copy(obs_hbm, raw.at[2], in_sem.at[2]),
    ]
    settings = [
        pltpu.make_async_copy(angles_hbm, angles, in_sem.at[3]),
        pltpu.make_async_copy(kinds_hbm, kinds, in_sem.at[4]),
    ]
    for copy in loads + settings:
        copy.start()

    def coefs(layer, q):
        row = slice(layer * 24 + q, layer * 24 + q + 1)
        return cos_tab[row, :], sy_tab[row, :], sz_tab[row, :]

    def kron(value, out_bits, in_bits, layer, qubits):
        real, imag = value
        for position, q in qubits:
            cosine, sy, sz = coefs(layer, q)
            if out_bits.shape[1] > 128:
                cosine, sy, sz = (jnp.concatenate([v, v], axis=1) for v in (cosine, sy, sz))
            b_out = (out_bits >> position) & 1
            b_in = (in_bits >> position) & 1
            same = b_out == b_in
            a = jnp.where(same, cosine, sy * (b_in - b_out).astype(F32))
            b = jnp.where(same, sz * (1 - 2 * b_out).astype(F32), 0.0)
            if real is None:
                real, imag = a, b
            else:
                real, imag = real * a - imag * b, real * b + imag * a
        return real, imag

    def build_lane(ref, layer):
        j = lax.broadcasted_iota(jnp.int32, (128, 128), 0)
        k = lax.broadcasted_iota(jnp.int32, (128, 128), 1)
        real, imag = kron((None, None), k, j, layer, list(enumerate(LANE_QUBITS)))
        for i, (re, im) in enumerate(zip(cut(real), cut(imag))):
            ref[i, 0:128, 0:128] = re
            ref[i, 128:256, 128:256] = re
            ref[i, 0:128, 128:256] = im
            ref[i, 128:256, 0:128] = -im

    def build_chunk_lane(ref, layer):
        j = lax.broadcasted_iota(jnp.int32, (128, 128), 0)
        k = lax.broadcasted_iota(jnp.int32, (128, 128), 1)
        qubits = [(p, q) for p, q in enumerate(LANE_QUBITS) if p != 4]
        real, imag = kron((None, None), k, j, layer, qubits)
        part_in, part_out = (j >> 4) & 1, (k >> 4) & 1
        mixed = jnp.where(part_in == part_out, real, jnp.where(part_out == 1, imag, -imag))
        ref[0], ref[1] = cut(mixed)

    def build_rows(ref, layer, qubits):
        places = list(enumerate(qubits))
        j = lax.broadcasted_iota(jnp.int32, (32, 256), 0)
        k = lax.broadcasted_iota(jnp.int32, (32, 256), 1)
        base = kron((None, None), j, k, layer, places[:5])

        def body(block, carry):
            real, imag = kron(base, j + block * 32, k, layer, places[5:])
            at = pl.ds(pl.multiple_of(block * 32, 32), 32)
            for i, (re, im) in enumerate(zip(cut(real), cut(imag))):
                ref[0, i, at, :] = re
                ref[1, i, at, :] = im
            return carry

        lax.fori_loop(0, 8, body, 0)

    def apply_lanes(x, ref):
        return mm(cut(x), (ref[0], ref[1]))

    def apply_rows(x, ref):
        x = cut(x)
        a, b = mm((ref[0, 0], ref[0, 1]), x), mm((ref[1, 0], ref[1, 1]), x)
        return jnp.concatenate([a[:, :128] - b[:, 128:], a[:, 128:] + b[:, :128]], axis=1)

    def apply_chunk_rows(x, ref):
        x = cut(x)
        return mm((ref[0, 0], ref[0, 1]), x) + times_i(mm((ref[1, 0], ref[1, 1]), x))

    def split(x):
        return x[:, :128], x[:, 128:]

    for copy in loads:
        copy.wait()
    for i in range(3):
        raw[i] = repack(raw[i])
    send_a[0], send_b[0] = to_chunks(raw[0], raw[1])
    send_a[1] = raw[2]

    def keep_own(source, target):
        target[:, pl.ds(me, 1), :] = source[:, pl.ds(me, 1), :]

    keep_own(send_a, recv_a)
    keep_own(send_b, recv_b)

    pl.semaphore_wait(barrier, 255)

    def exchange(source, target, slot):
        def act(d):
            pltpu.make_async_remote_copy(
                src_ref=source.at[:, pl.ds(d, 1), :],
                dst_ref=target.at[:, pl.ds(me, 1), :],
                send_sem=send_sems.at[slot],
                recv_sem=recv_sems.at[slot],
                device_id=(d,),
                device_id_type=MESH,
            ).start()

        to_all(act)

    def exchanged(source, target, slot):
        return pltpu.make_async_remote_copy(
            src_ref=source.at[:, pl.ds(0, 255), :],
            dst_ref=target.at[:, pl.ds(0, 255), :],
            send_sem=send_sems.at[slot],
            recv_sem=recv_sems.at[slot],
            device_id=(me,),
            device_id_type=MESH,
        )

    exchange(send_a, recv_a, 0)
    exchange(send_b, recv_b, 1)
    out_a = exchanged(send_a, recv_a, 0)
    out_b = exchanged(send_b, recv_b, 1)

    for copy in settings:
        copy.wait()
    theta[...] = jnp.zeros_like(theta)
    kind_tab[...] = jnp.zeros_like(kind_tab)
    picks = {}
    for layer in range(2):
        for q in range(QUBITS):
            kind = kinds[layer, q]
            picks[layer, q] = [jnp.where(kind == k, 1.0, 0.0).astype(F32) for k in range(3)]
            angle = jnp.where(
                kind == 0, angles[layer, 0], jnp.where(kind == 1, angles[layer, 1], angles[layer, 2])
            )
            row = layer * 24 + q
            theta[row : row + 1, :] = jnp.full((1, 128), 0.5 * angle, F32)
            kind_tab[row : row + 1, :] = jnp.full((1, 128), kind, jnp.int32)
    cos_tab[...] = jnp.cos(theta[...])
    sines = jnp.sin(theta[...])
    is_z = kind_tab[...] == 2
    sy_tab[...] = jnp.where(is_z, 0.0, sines)
    sz_tab[...] = jnp.where(is_z, sines, 0.0)

    build_chunk_lane(chunk_lane1, 1)
    build_rows(away1, 1, AWAY_ROWS)
    build_rows(away0, 0, AWAY_ROWS)
    build_lane(lane1, 1)
    build_rows(home1, 1, HOME_ROWS)

    scale = 2.0 / math.sqrt(1 << QUBITS)

    acc = {(layer, k): jnp.zeros((8, 128), F32) for layer in range(2) for k in range(3)}

    def tally(layer, qubits, values):
        for q, (y_part, z_part) in zip(qubits, values):
            pick = picks[layer, q]
            acc[layer, 0] = acc[layer, 0] + pick[0] * y_part
            acc[layer, 1] = acc[layer, 1] + pick[1] * y_part
            acc[layer, 2] = acc[layer, 2] + pick[2] * z_part

    spots = [(1, p) for p in range(7)] + [(0, p) for p in range(8)]
    local = list(LANE_QUBITS) + list(HOME_ROWS)
    sign = entangle(me, ALL_PAIRS)
    ket = (raw[0] * sign, raw[1] * sign)
    bra = tuple(raw[2] * scale * part for part in ket)
    tally(1, local, home_terms(bra, ket, spots))
    local_sign = entangle(me, LOCAL_PAIRS)
    sign2 = jnp.concatenate([local_sign, local_sign], axis=1)

    def home_layer(state):
        x = jnp.concatenate(state, axis=1)
        return split(apply_rows(apply_lanes(x, lane1), home1) * sign2)

    inside = [(q, s) for q, s in zip(local, spots) if q not in (0, 14)]
    tally(0, [q for q, _ in inside], home_terms(home_layer(bra), home_layer(ket), [s for _, s in inside]))

    def give_sums():
        lane8 = lax.broadcasted_iota(jnp.int32, (8, 128), 1)
        mine = jnp.zeros((8, 128), F32)
        for layer in range(2):
            for k in range(3):
                value = 0.5 * jnp.sum(acc[layer, k], keepdims=True)
                mine = mine + jnp.where(lane8 == 3 * layer + k, value, 0.0)
        part[...] = mine
        from_plane[pl.ds(plane, 1)] = mine[None]

        def hand_over(d, spot):
            pltpu.make_async_remote_copy(
                src_ref=part, dst_ref=from_plane.at[plane], send_sem=send_sems.at[4], recv_sem=recv_sems.at[4],
                device_id=(d,), device_id_type=MESH,
            ).start()

        to_plane(hand_over)

    row_spots = [(0, p) for p in range(8)]

    def visit(chunk, arrived, source, send, recv, slot):
        start_sign = entangle(me, ALL_PAIRS, chunk)
        away_sign = entangle(me, AWAY_PAIRS, chunk)
        if chunk == 0:
            arrived.wait_recv()
        obs = recv_a[1]
        keep = lane_bit4()
        obs = jnp.where(keep, obs, up(obs)) if chunk == 0 else jnp.where(keep, down(obs), obs)
        obs = obs * scale
        if chunk == 1:
            arrived.wait_recv()
        ket = source[0] * start_sign
        bra = obs * ket

        def away_layer(x):
            x = mm(cut(x), (chunk_lane1[0], chunk_lane1[1]))
            return apply_chunk_rows(x, away1) * away_sign

        def leave(bra_x):
            send[0] = apply_chunk_rows(bra_x, away0)
            keep_own(send, recv)
            exchange(send, recv, slot)

        def take_terms(bra_x, ket_x):
            tally(1, AWAY_ROWS, chunk_terms(bra, ket, row_spots))
            tally(0, list(AWAY_ROWS) + [0, 14], chunk_terms(bra_x, ket_x, row_spots + [(1, 0), (1, 6)]))

        if chunk == 0:
            bra_x = away_layer(bra)
            leave(bra_x)
            take_terms(bra_x, away_layer(ket))
        else:
            x = jnp.concatenate([bra, ket], axis=0)
            x = mm(cut(x), (chunk_lane1[0], chunk_lane1[1]))
            x = cut(jnp.concatenate([x[:256], x[256:]], axis=1))
            a, b = mm((away1[0, 0], away1[0, 1]), x), mm((away1[1, 0], away1[1, 1]), x)
            bra_x = (a[:, :128] + times_i(b[:, :128])) * away_sign
            ket_x = (a[:, 128:] + times_i(b[:, 128:])) * away_sign
            take_terms(bra_x, ket_x)
            give_sums()
            leave(bra_x)

    visit(0, out_a, recv_a, send_c, recv_c, 2)
    out_c = exchanged(send_c, recv_c, 2)
    visit(1, out_b, recv_b, send_d, recv_d, 3)
    out_d = exchanged(send_d, recv_d, 3)

    third = pltpu.make_async_remote_copy(
        src_ref=from_plane.at[pl.ds(0, 31)], dst_ref=from_plane.at[pl.ds(0, 31)],
        send_sem=send_sems.at[4], recv_sem=recv_sems.at[4], device_id=(me,), device_id_type=MESH,
    )
    build_lane(lane0, 0)
    build_rows(home0, 0, HOME_ROWS)
    rest_sign = entangle(me, REST_PAIRS)
    rest2 = jnp.concatenate([rest_sign, rest_sign], axis=1)

    third.wait_recv()
    summed = jnp.sum(from_plane[...], axis=0)
    part_z[...] = summed
    from_z[pl.ds(z, 1)] = summed[None]
    for dz in (4, 3, 5, 2, 6, 1, 7):
        pltpu.make_async_remote_copy(
            src_ref=part_z, dst_ref=from_z.at[z], send_sem=send_sems.at[5], recv_sem=recv_sems.at[5],
            device_id=(((z + dz) % 8) * 32 + plane,), device_id_type=MESH,
        ).start()
    fourth = pltpu.make_async_remote_copy(
        src_ref=from_z.at[pl.ds(0, 7)], dst_ref=from_z.at[pl.ds(0, 7)],
        send_sem=send_sems.at[5], recv_sem=recv_sems.at[5], device_id=(me,), device_id_type=MESH,
    )

    cosine, sy, sz = coefs(1, 4)
    out_c.wait_recv()
    low = apply_chunk_rows(recv_c[0], home1)
    out_d.wait_recv()
    high = apply_chunk_rows(recv_d[0], home1)
    low, high = (
        cosine * low + sy * high + sz * times_i(low),
        cosine * high - sy * low - sz * times_i(high),
    )
    x2 = jnp.concatenate(from_chunks(low, high), axis=1) * rest2
    x2 = apply_rows(apply_lanes(x2, lane0), home0)
    bra_ref[0], bra_ref[1] = split(x2)

    fourth.wait_recv()
    grads_ref[...] = jnp.sum(from_z[...], axis=0)
    for copy in (out_a, out_b, out_c, out_d, third, fourth):
        copy.wait_send()


def finish(state, sums, bra_hbm, grads_ref, raw, out_sem):
    stores = []
    for i in range(2):
        raw[i] = repack(state[i])
        stores.append(pltpu.make_async_copy(raw.at[i], bra_hbm.at[:, i, :], out_sem.at[i]))
        stores[i].start()
    total = sums[0:1, :]
    grads_ref[...] = jnp.concatenate([total[:, 0:3], total[:, 3:6]], axis=0)
    for copy in stores:
        copy.wait()


def on_device(ket_state, observable, angles, gate_kinds):
    ket = ket_state.reshape(2, 256, 128).transpose(1, 0, 2)
    obs = observable.reshape(256, 128)
    main_memory = pl.BlockSpec(memory_space=pltpu.HBM)
    vmem = lambda *shape, dtype=F32: pltpu.VMEM(shape, dtype)
    half = lambda *shape: pltpu.VMEM(shape, jnp.bfloat16)
    on_chip = pl.BlockSpec(memory_space=pltpu.VMEM)
    state, sums = pl.pallas_call(
        kernel,
        out_shape=(
            jax.ShapeDtypeStruct((2, 256, 128), F32),
            jax.ShapeDtypeStruct((8, 128), F32),
        ),
        in_specs=[main_memory] * 4,
        out_specs=(on_chip, on_chip),
        scratch_shapes=[
            pltpu.SMEM((2, 3), F32), pltpu.SMEM((2, 32), jnp.int32),
            vmem(3, 256, 128),
            vmem(2, 256, 128), vmem(1, 256, 128), vmem(2, 256, 128), vmem(1, 256, 128),
            vmem(1, 256, 128), vmem(1, 256, 128), vmem(1, 256, 128), vmem(1, 256, 128),
            vmem(48, 128), vmem(48, 128, dtype=jnp.int32),
            vmem(48, 128), vmem(48, 128), vmem(48, 128),
            half(2, 256, 256), half(2, 256, 256), half(2, 128, 128),
            half(2, 2, 256, 256), half(2, 2, 256, 256), half(2, 2, 256, 256), half(2, 2, 256, 256),
            vmem(8, 128), vmem(8, 8, 128), vmem(8, 128), vmem(32, 8, 128),
            pltpu.SemaphoreType.DMA((5,)),
            pltpu.SemaphoreType.DMA((6,)), pltpu.SemaphoreType.DMA((6,)),
        ],
        compiler_params=pltpu.CompilerParams(
            collective_id=0, has_side_effects=True, vmem_limit_bytes=16 << 20
        ),
    )(*(pltpu.with_memory_space_constraint(v, pltpu.HBM) for v in (ket, obs, angles, gate_kinds)))
    bra, grads = pl.pallas_call(
        finish,
        out_shape=(
            jax.ShapeDtypeStruct((256, 2, 128), F32),
            jax.ShapeDtypeStruct((2, 3), F32),
        ),
        in_specs=[on_chip, on_chip],
        out_specs=(main_memory, on_chip),
        scratch_shapes=[vmem(2, 256, 128), pltpu.SemaphoreType.DMA((2,))],
        compiler_params=pltpu.CompilerParams(vmem_limit_bytes=4 << 20),
    )(state, sums)
    return bra.transpose(1, 0, 2).reshape(2, 32768), grads


def solution(mesh):
    return jax.shard_map(
        on_device,
        mesh=mesh,
        in_specs=(P(None, "amp"), P("amp"), P(), P()),
        out_specs=(P(None, "amp"), P()),
        check_vma=False,
    )
```
